32 devices in a mesh: ctx: 8 (over y, x, core), head: 4 (over z).
Axes of the slice: x: 2, y: 2, z: 4, core: 2. Of those that a mesh axis runs over, the one named last changes fastest.
Arguments:
- q_latent: bfloat16 [2048, 1536], P('ctx', 'head'), may hold values from -70 to 70
- kv_latent: bfloat16 [2048, 576], P('ctx', 'head'), may hold values from -6 to 6
- w_query: bfloat16 [1536, 12288], P(None, 'head'), may hold values from -0.15625 to 0.15625
- w_key: bfloat16 [512, 8192], P(None, 'head'), may hold values from -0.25 to 0.25
- w_value: bfloat16 [512, 8192], P(None, 'head'), may hold values from -0.25 to 0.25
- d_out: bfloat16 [2048, 8192], P('ctx', 'head'), may hold values from -6 to 6
Outputs:
- attn_out: bfloat16 [2048, 8192], P('ctx', 'head')
- grad_qlat: float32 [2048, 1536], P('ctx', 'head')
- grad_kvlat: float32 [2048, 576], P('ctx', 'head')
The draws below stay inside these ranges and needn't reach their ends.
All inputs are finite; a program needn't handle non-finite values.
Results may differ from the reference program's by a relative error of at most 0.023.
The reference program's roundings to bfloat16 on the way (of `queries`, `probs_b`, `dscore` and `grad_query`) count: a program that leaves them out, or rounds other values in their place, can miss the bound.
Values may be sent and summed in bfloat16 or wider, within the bound.
A program may use at most 128 MiB of HBM per device.

```python
import jax
import jax.numpy as jnp
from jax import lax

QL = 1536
KVL = 512
ROPE = 64
NOPE = 128
VDIM = 128
HEAD_DEV = 16
TOK_DEV = 256
HEADS = 64
TOKENS = 2048
N_CTX = 8
N_HEAD = 4


def draw_q_latent(key, part):
    base_key = jax.random.fold_in(jax.random.fold_in(key, 11), 0)
    values = jax.random.normal(base_key, (TOKENS, QL), jnp.float32)
    return jnp.clip(values, -6.0, 6.0).astype(jnp.bfloat16)


def steps_of(key, dims, shards, low, high):
    def one(axis_at, parts):
        heights = jax.random.uniform(jax.random.fold_in(jax.random.fold_in(key, 6), axis_at), (parts,), jnp.float32, low / len(shards), high / len(shards))
        return jnp.repeat(jnp.exp(heights), dims[axis_at] // parts).reshape((-1,) + (1,) * (len(dims) - axis_at - 1))

    factor_of = one(*shards[0])
    for cut in shards[1:]:
        factor_of = factor_of * one(*cut)
    return factor_of


def noise(stream_key, dims, deviation, reach, cuts=(), held_as=jnp.bfloat16):
    loudness = steps_of(stream_key, dims, cuts, -0.22, 0.18) if cuts else 1.0
    result = jax.random.normal(stream_key, dims, jnp.float32) * deviation * loudness
    return jnp.minimum(jnp.maximum(result, -reach), reach).astype(held_as)


def setup_inputs(seed: int = 0) -> dict:
    streams_of = jax.random.split(jax.random.key(seed), 7)
    return {
        "q_latent": draw_q_latent(jax.random.fold_in(streams_of[6], 71), 0),
        "kv_latent": noise(streams_of[1], (TOKENS, KVL + ROPE), 1.0, 6.0, ((0, 8), (1, 4))),
        "w_query": noise(streams_of[2], (QL, HEADS * (NOPE + ROPE)), QL ** -0.5, 0.15625, ((1, 4),)),
        "w_key": noise(streams_of[3], (KVL, HEADS * NOPE), KVL ** -0.5, 0.25, ((1, 4),)),
        "w_value": noise(streams_of[4], (KVL, HEADS * VDIM), KVL ** -0.5, 0.25, ((1, 4),)),
        "d_out": noise(streams_of[5], (TOKENS, HEADS * VDIM), 1.0, 6.0, ((0, 8), (1, 4))),
    }


def to_float(array):
    return array.astype(jnp.float32)


def shift_down(array):
    return jnp.concatenate([jnp.zeros_like(array[:1]), array[:-1]], 0)


def shift_up(array):
    return jnp.concatenate([array[1:], jnp.zeros_like(array[:1])], 0)


def reference(q_latent, kv_latent, w_query, w_key, w_value, d_out):
    group_count = N_HEAD
    per_group = HEAD_DEV
    block_count = N_CTX
    block_rows = TOK_DEV
    width = NOPE + ROPE
    softmax_scale = width ** -0.5
    query_w = w_query.reshape(QL, group_count, per_group * width).transpose(1, 0, 2)
    key_w = w_key.reshape(KVL, group_count, per_group * NOPE).transpose(1, 0, 2)
    value_w = w_value.reshape(KVL, group_count, per_group * VDIM).transpose(1, 0, 2)
    grad_groups = d_out.reshape(TOKENS, group_count, per_group * VDIM).transpose(1, 0, 2)
    rope_keys = kv_latent[:, KVL:].reshape(block_count, block_rows, ROPE)
    rope_all = jnp.concatenate([shift_down(rope_keys), rope_keys], 1)
    query_pos = jnp.arange(block_rows)[:, None]
    key_pos = jnp.arange(2 * block_rows)[None, :]
    block_idx = jnp.arange(block_count)[:, None, None]
    visible = jnp.where(key_pos < block_rows, block_idx > 0, key_pos - block_rows <= query_pos)
    latent_main = kv_latent[:, :KVL]

    def group_step(carry, inputs):
        wq_group, wk_group, wv_group, grad_group = inputs
        queries = jnp.dot(q_latent, wq_group, preferred_element_type=jnp.float32).astype(jnp.bfloat16)
        queries = queries.reshape(block_count, block_rows, per_group, width)
        keys_nope = jnp.dot(latent_main, wk_group, preferred_element_type=jnp.float32).astype(jnp.bfloat16)
        keys_nope = keys_nope.reshape(block_count, block_rows, per_group, NOPE)
        values = jnp.dot(latent_main, wv_group, preferred_element_type=jnp.float32).astype(jnp.bfloat16)
        values = values.reshape(block_count, block_rows, per_group, VDIM)
        keys_all = jnp.concatenate([shift_down(keys_nope), keys_nope], 1)
        values_all = jnp.concatenate([shift_down(values), values], 1)
        query_nope = queries[..., :NOPE]
        query_rope = queries[..., NOPE:]
        scores = jnp.einsum("nqhd,nkhd->nhqk", to_float(query_nope), to_float(keys_all))
        scores = (scores + jnp.einsum("nqhr,nkr->nhqk", to_float(query_rope), to_float(rope_all))) * softmax_scale
        mask = visible[:, None]
        scores = jnp.where(mask, scores, jnp.float32(-1e30))
        maxima = jnp.max(scores, -1, keepdims=True)
        expons = jnp.where(mask, jnp.exp(scores - maxima), jnp.float32(0.0))
        probs = expons / jnp.sum(expons, -1, keepdims=True)
        probs_b = probs.astype(jnp.bfloat16)
        output = jnp.einsum("nhqk,nkhd->nqhd", to_float(probs_b), to_float(values_all)).astype(jnp.bfloat16)
        grad_out = grad_group.reshape(block_count, block_rows, per_group, VDIM)
        dprob = jnp.einsum("nqhd,nkhd->nhqk", to_float(grad_out), to_float(values_all))
        row_dot = jnp.sum(to_float(grad_out) * to_float(output), -1).transpose(0, 2, 1)[..., None]
        dscore = (probs * (dprob - row_dot) * softmax_scale).astype(jnp.bfloat16)
        grad_qnope = jnp.einsum("nhqk,nkhd->nqhd", to_float(dscore), to_float(keys_all))
        grad_qrope = jnp.einsum("nhqk,nkr->nqhr", to_float(dscore), to_float(rope_all))
        grad_query = jnp.concatenate([grad_qnope, grad_qrope], -1).astype(jnp.bfloat16)
        grad_query = grad_query.reshape(TOKENS, per_group * width)
        grad_qgroup = jnp.dot(grad_query, wq_group.T, preferred_element_type=jnp.float32)
        grad_knope = jnp.einsum("nhqk,nqhd->nkhd", to_float(dscore), to_float(query_nope)).astype(jnp.bfloat16)
        grad_krope = jnp.einsum("nhqk,nqhr->nkhr", to_float(dscore), to_float(query_rope)).astype(jnp.bfloat16)
        grad_value = jnp.einsum("nhqk,nqhd->nkhd", to_float(probs_b), to_float(grad_out)).astype(jnp.bfloat16)

        def project(knope_part, krope_part, value_part):
            main_cols = jnp.dot(knope_part.reshape(TOKENS, per_group * NOPE), wk_group.T, preferred_element_type=jnp.float32)
            main_cols = main_cols + jnp.dot(value_part.reshape(TOKENS, per_group * VDIM), wv_group.T, preferred_element_type=jnp.float32)
            rope_cols = jnp.sum(to_float(krope_part), axis=2).reshape(TOKENS, ROPE)
            return jnp.concatenate([main_cols, rope_cols], -1)

        own_part = project(grad_knope[:, block_rows:], grad_krope[:, block_rows:], grad_value[:, block_rows:])
        next_part = project(shift_up(grad_knope[:, :block_rows]), shift_up(grad_krope[:, :block_rows]), shift_up(grad_value[:, :block_rows]))
        carry = (carry[0] + grad_qgroup, carry[1] + own_part + next_part)
        return carry, output.reshape(TOKENS, per_group * VDIM)

    start = (jnp.zeros((TOKENS, QL), jnp.float32), jnp.zeros((TOKENS, KVL + ROPE), jnp.float32))
    grads, outputs = lax.scan(group_step, start, (query_w, key_w, value_w, grad_groups))
    attn_out = outputs.transpose(1, 0, 2).reshape(TOKENS, HEADS * VDIM)
    return attn_out, grads[0], grads[1]
```

```python
import functools
import math

import jax
import jax.numpy as jnp
from jax import lax
from jax.experimental import pallas as pl
from jax.experimental.pallas import tpu as pltpu
from jax.sharding import PartitionSpec as P

KVL = 512
ROPE = 64
NOPE = 128
VDIM = 128
WIDTH = NOPE + ROPE
SCALE = WIDTH ** (-0.5)
F32 = jnp.float32
BF16 = jnp.bfloat16
MESH = pl.DeviceIdType.MESH


def nn(a, b):
    return jnp.dot(a, b, preferred_element_type=F32)


def nt(a, b):
    return lax.dot_general(a, b, (((1,), (1,)), ((), ())), preferred_element_type=F32)


def kernel(
    n_ctx, n_head,
    q_ref, kv_ref, do_ref, wq_hbm, wk_hbm, wv_hbm,
    out_ref, gq_ref, gkv_ref,
    wq, wk, wv, wkt, wvt, dot_t, q_in, kv_in, kv_prev, lat_t, q_acc, q_b,
    keys_t, values_t, s_buf, dp_buf, p_buf, pb_all, ds_all, gq_t, gk_t, gv_t, krope, back_out, back_in,
    rq_out, rq_right, rq_left, rkv_out, rkv_right, rkv_left, gkv_own, stage_right, stage_left,
    bias, w_sem, kv_r, kv_l, kv_recv, q_r, q_l, q_recv, p_send, p_recv,
    b_send, b_recv, rq_send, rq_rr, rq_rl, rkv_send, rkv_rr, rkv_rl,
):
    ctx = lax.axis_index("ctx")
    me = lax.axis_index("head")
    last = n_head - 1
    rows, q_cols = q_ref.shape
    part_rows = rows // CHUNKS
    kv_cols = kv_ref.shape[0]
    heads = wk.shape[1] // NOPE
    after = {"ctx": lax.rem(ctx + 1, n_ctx)}
    before = {"ctx": lax.rem(ctx + n_ctx - 1, n_ctx)}
    right = {"head": jnp.minimum(me + 1, last)}
    left = {"head": jnp.maximum(me - 1, 0)}
    has_right = me < last
    has_left = me > 0

    loads = [
        pltpu.make_async_copy(src, dst, w_sem.at[i])
        for i, (src, dst) in enumerate(((wk_hbm, wk), (wv_hbm, wv), (wq_hbm, wq)))
    ]
    for load in loads:
        load.start()

    barrier = pltpu.get_barrier_semaphore()

    @pl.when(has_right)
    def _():
        pl.semaphore_signal(barrier, inc=1, device_id=right, device_id_type=MESH)

    @pl.when(has_left)
    def _():
        pl.semaphore_signal(barrier, inc=1, device_id=left, device_id_type=MESH)

    pl.semaphore_signal(barrier, inc=1, device_id=after, device_id_type=MESH)
    pl.semaphore_signal(barrier, inc=1, device_id=before, device_id_type=MESH)
    pl.semaphore_wait(barrier, 2 + jnp.minimum(me, 1) + jnp.minimum(last - me, 1))

    def copy_of(src, dst, send_sem, recv_sem, device):
        return pltpu.make_async_remote_copy(
            src_ref=src, dst_ref=dst, send_sem=send_sem, recv_sem=recv_sem,
            device_id=device, device_id_type=MESH,
        )

    class Gather:
        def __init__(self, own, slots, send_r, send_l, recv):
            self.own, self.slots, self.recv = own, slots, recv
            self.send_r, self.send_l = send_r, send_l

        def moves(self, t, act):
            @pl.when(has_right & (me >= t))
            def _():
                owner = me - t
                src = self.own if t == 0 else self.slots(owner)
                act(copy_of(src, self.slots(owner), self.send_r(t), self.recv(owner), right))

            @pl.when(has_left & (me + t <= last))
            def _():
                owner = me + t
                src = self.own if t == 0 else self.slots(owner)
                act(copy_of(src, self.slots(owner), self.send_l(t), self.recv(owner), left))

        def start(self, t):
            if t < last:
                self.moves(t, lambda copy: copy.start())

        def each(self, t, act):
            @pl.when(me - 1 - t >= 0)
            def _():
                act(me - 1 - t)

            @pl.when(me + 1 + t <= last)
            def _():
                act(me + 1 + t)

        def arrive(self, t, act=None):
            def wait(owner):
                slot = self.slots(owner)
                copy_of(slot, slot, self.send_r(0), self.recv(owner), right).wait_recv()
                if act is not None:
                    act(owner)

            self.each(t, wait)
            self.start(t + 1)

        def finish(self):
            for t in range(last):
                self.moves(t, lambda copy: copy.wait_send())

    def pass_on(owner, src):
        copy_of(src, kv_prev.at[owner], p_send.at[owner], p_recv.at[owner], after).start()

    kv_gather = Gather(kv_ref, lambda i: kv_in.at[i], lambda t: kv_r.at[t], lambda t: kv_l.at[t], lambda i: kv_recv.at[i])
    q_gathers = [
        Gather(
            q_ref.at[pl.ds(c * part_rows, part_rows), :],
            lambda i, c=c: q_in.at[c, i],
            lambda t, c=c: q_r.at[c, t],
            lambda t, c=c: q_l.at[c, t],
            lambda i, c=c: q_recv.at[c, i],
        )
        for c in range(CHUNKS)
    ]
    kv_gather.start(0)
    q_gathers[0].start(0)
    pass_on(me, kv_ref)
    kv_in[me] = kv_ref[...]

    key_pos = lax.broadcasted_iota(jnp.int32, (part_rows, part_rows), 1)
    query_pos = lax.broadcasted_iota(jnp.int32, (part_rows, part_rows), 0)
    bias[...] = jnp.where(key_pos <= query_pos, F32(0.0), F32(-1e30))
    prev_mask = jnp.where(ctx == 0, F32(-1e30), F32(0.0))
    for c in range(CHUNKS - 1):
        seen = rows + (c + 1) * part_rows
        unseen = jnp.zeros((heads, part_rows, 2 * rows - seen), BF16)
        pb_all[:, c * part_rows:(c + 1) * part_rows, seen:] = unseen
        ds_all[:, c * part_rows:(c + 1) * part_rows, seen:] = unseen

    def turn(src, dst):
        @pl.loop(0, heads // 2)
        def _(j):
            for u in range(2):
                at = pl.multiple_of((2 * j + u) * NOPE, NOPE)
                dst[pl.ds(at, NOPE), :] = src[:, pl.ds(at, NOPE)].T

    def kv_step(t):
        kv_gather.arrive(t, lambda owner: pass_on(owner, kv_in.at[owner]))

    def q_step(c, t):
        q_gathers[c].arrive(t)

    def add_queries(c, block, owner, first=False):
        at = pl.multiple_of(owner * q_cols, q_cols)
        tile = 4 * WIDTH

        @pl.loop(0, wq.shape[1] // tile)
        def _(j):
            cols = pl.ds(pl.multiple_of(j * tile, tile), tile)
            part = nn(block[...], wq[pl.ds(at, q_cols), cols])
            if first:
                q_acc[:, cols] = part
            else:
                q_acc[:, cols] += part

    def own_queries(c):
        add_queries(c, q_ref.at[pl.ds(c * part_rows, part_rows), :], me, True)

    def add_arrived(c, t):
        q_gathers[c].each(t, lambda owner: add_queries(c, q_in.at[c, owner], owner))

    def finish_queries(c):
        q_b[c * part_rows:(c + 1) * part_rows, :] = q_acc[...].astype(BF16)

    def assemble(parts, row):
        span = slice(row, row + rows)
        if kv_cols % 16 == 0:
            for i in range(n_head):
                lat_t[i * kv_cols:(i + 1) * kv_cols, span] = parts[i]
            return
        width = n_head * kv_cols
        total = None
        for i in range(n_head):
            dst = lax.broadcasted_iota(jnp.int32, (width, kv_cols), 0)
            src = lax.broadcasted_iota(jnp.int32, (width, kv_cols), 1) + i * kv_cols
            place = jnp.where(src == dst, F32(1.0), F32(0.0)).astype(BF16)
            term = nn(place, parts[i])
            total = term if total is None else total + term
        lat_t[:, span] = total.astype(BF16)

    def expand(row):
        tile = 4 * NOPE
        span = slice(row, row + rows)

        @pl.loop(0, heads // 4)
        def _(j):
            cols = pl.ds(pl.multiple_of(j * tile, tile), tile)
            main_t = lat_t[:KVL, span]
            keys_t[cols, span] = nn(wkt[cols, :], main_t).astype(BF16)
            values_t[cols, span] = nn(wvt[cols, :], main_t).astype(BF16)

    def window(h, odd):
        first = (h - 1 if odd else h) * WIDTH + (NOPE if odd else 0)
        return pl.ds(pl.multiple_of(first, NOPE), WIDTH + ROPE)

    def columns(h):
        return pl.ds(pl.multiple_of(h * NOPE, NOPE), NOPE)

    def seen_by(c):
        return rows + (c + 1) * part_rows

    def span_of(c):
        return slice(c * part_rows, (c + 1) * part_rows)

    def pieces(c):
        return [
            (slice(r, r + PIECE), slice(c * part_rows + r, c * part_rows + r + PIECE))
            for r in range(0, part_rows, PIECE)
        ]

    def score_stage(c, h, odd):
        seen = seen_by(c)
        query = q_b[span_of(c), window(h, odd)]
        key = [keys_t[columns(h), :seen], lat_t[KVL:, :seen]]
        pad = [jnp.zeros((ROPE, seen), BF16)]
        s_buf[:, :seen] = nn(query, jnp.concatenate(pad + key if odd else key + pad, 0))

    def softmax_stage(c, h):
        seen = seen_by(c)
        dp_buf[:, :seen] = nn(do_ref[span_of(c), columns(h)], values_t[columns(h), :seen])
        for sub, row in pieces(c):
            scores = [s_buf[sub, :rows] + prev_mask]
            if c > 0:
                scores.append(s_buf[sub, rows:seen - part_rows])
            scores.append(s_buf[sub, seen - part_rows:seen] + bias[sub, :])
            scores = jnp.concatenate(scores, 1)
            top = jnp.max(scores, 1, keepdims=True)
            expons = jnp.exp2((scores - top) * F32(SCALE * math.log2(math.e)))
            probs = expons * (F32(1.0) / jnp.sum(expons, 1, keepdims=True))
            p_buf[sub, :seen] = probs
            pb_all[h, row, :seen] = probs.astype(BF16)

    def output_stage(c, h):
        seen = seen_by(c)
        span = span_of(c)
        cols = columns(h)
        result = nt(pb_all[h, span, :seen], values_t[cols, :seen]).astype(BF16)
        out_ref[span, cols] = result
        row_dot = jnp.sum(do_ref[span, cols].astype(F32) * result.astype(F32), 1, keepdims=True)
        for sub, row in pieces(c):
            dscore = p_buf[sub, :seen] * (dp_buf[sub, :seen] - row_dot[sub]) * F32(SCALE)
            ds_all[h, row, :seen] = dscore.astype(BF16)

    def gradient_stage(c, h, odd, valid):
        seen = seen_by(c)
        span = span_of(c)
        cols = columns(h)
        key = jnp.concatenate([keys_t[cols, :seen], lat_t[KVL:, :seen]], 0)
        q_at = pl.ds(pl.multiple_of(h * WIDTH, ROPE), WIDTH)
        gq_t[q_at, span] = nt(key, ds_all[h, span, :seen]).astype(BF16)
        if c + 1 < CHUNKS:
            return
        query_t = q_b[:, window(h, odd)].T
        query_t = query_t[ROPE:] if odd else query_t[:WIDTH]
        g_key = nn(query_t, ds_all[h])
        gk_t[cols, :] = g_key[:NOPE].astype(BF16)
        g_rope = g_key[NOPE:].astype(BF16).astype(F32)
        krope[...] += g_rope if valid is None else jnp.where(valid, g_rope, F32(0.0))
        gv_t[cols, :] = nn(dot_t[cols, :], pb_all[h]).astype(BF16)

    def attention(c, hooks):
        trips = heads // 2
        count = len(hooks) + 1

        @pl.loop(0, trips)
        def _(t):
            for i, hook in enumerate(hooks):
                pl.when(t == trips * (i + 1) // count)(hook)
            for u in range(2):
                odd = u == 1
                step = 2 * t + u
                gradient_stage(c, jnp.maximum(step - 3, 0 if odd else 1), not odd, step >= 3)
                output_stage(c, jnp.maximum(step - 2, 0))
                softmax_stage(c, jnp.maximum(step - 1, 0))
                score_stage(c, step, odd)

        gradient_stage(c, heads - 3, True, None)
        output_stage(c, heads - 2)
        softmax_stage(c, heads - 1)
        gradient_stage(c, heads - 2, False, None)
        output_stage(c, heads - 1)
        gradient_stage(c, heads - 1, True, None)

    class Reduce:
        def __init__(self, part, out, in_right, in_left, send, recv_right, recv_left, stages):
            self.part, self.out, self.send = part, out, send
            self.ways = (
                (in_right, recv_right, right, stages[0], has_left),
                (in_left, recv_left, left, stages[1], has_right),
            )

        def step(self, tick):
            for way, (slots, recv, device, stage, joined) in enumerate(self.ways):
                lag = me if way == 0 else last - me
                owner = last - (tick - lag) if way == 0 else tick - lag

                @pl.when(tick >= lag)
                def _():
                    stage[...] = self.part(owner)

                    @pl.when(joined)
                    def _():
                        copy_of(slots(owner), slots(owner), self.send(owner), recv(owner), device).wait_recv()
                        stage[...] += slots(owner)[...].astype(F32)

                    self.out(owner)[...] = stage[...].astype(BF16)
                    copy_of(self.out(owner), slots(owner), self.send(owner), recv(owner), device).start()

        def total(self, stage):
            stage[...] = self.part(me)
            for slots, recv, device, _, joined in self.ways:
                @pl.when(joined)
                def _():
                    copy_of(slots(me), slots(me), self.send(me), recv(me), device).wait_recv()
                    stage[...] += slots(me)[...].astype(F32)

        def finish(self):
            for i in range(n_head):
                @pl.when(me != i)
                def _():
                    slot = self.out(i)
                    copy_of(slot, slot, self.send(i), self.send(i), right).wait_send()

    def query_part(c):
        def part(owner):
            at = pl.multiple_of(owner * q_cols, q_cols)
            return nn(wq[pl.ds(at, q_cols), :], gq_t[:, c * part_rows:(c + 1) * part_rows])

        return part

    def kv_part(owner):
        return gkv_own[pl.ds(pl.multiple_of(owner * kv_cols, 8), kv_cols), :]

    q_reduces = [
        Reduce(
            query_part(c),
            lambda i, c=c: rq_out.at[c, i],
            lambda i, c=c: rq_right.at[c, i],
            lambda i, c=c: rq_left.at[c, i],
            lambda i, c=c: rq_send.at[c, i],
            lambda i, c=c: rq_rr.at[c, i],
            lambda i, c=c: rq_rl.at[c, i],
            (stage_right, stage_left),
        )
        for c in range(CHUNKS)
    ]
    kv_stage = (gkv_ref, gkv_ref)
    kv_reduce = Reduce(
        kv_part,
        lambda i: rkv_out.at[i],
        lambda i: rkv_right.at[i],
        lambda i: rkv_left.at[i],
        lambda i: rkv_send.at[i],
        lambda i: rkv_rr.at[i],
        lambda i: rkv_rl.at[i],
        kv_stage,
    )

    loads[0].wait()
    turn(wk, wkt)
    if last > 0:
        kv_step(0)
    loads[1].wait()
    turn(wv, wvt)
    if last > 0:
        q_step(0, 0)
    turn(do_ref, dot_t)
    for t in range(1, last - 1):
        kv_step(t)
    loads[2].wait()
    own_queries(0)
    for t in range(1, last):
        add_arrived(0, t - 1)
        q_step(0, t)
        if t == max(1, last - 2):
            q_gathers[1].start(0)
    if last > 1:
        kv_step(last - 1)
    assemble([kv_in[i] for i in range(n_head)], rows)
    expand(rows)
    for i in range(n_head):
        copy_of(kv_ref, kv_prev.at[i], p_send.at[i], p_recv.at[i], after).wait_recv()
    assemble([kv_prev[i] for i in range(n_head)], 0)
    expand(0)
    if last > 0:
        add_arrived(0, last - 1)
    finish_queries(0)
    krope[...] = jnp.zeros_like(krope)
    if last > 0:
        q_step(1, 0)
    attention(0, [functools.partial(q_step, 1, t) for t in range(1, last)])
    if last > 0:
        q_reduces[0].step(0)
    own_queries(1)
    for t in range(last):
        add_arrived(1, t)
    finish_queries(1)
    attention(1, [functools.partial(q_reduces[0].step, t) for t in range(1, last)])

    def project(row):
        span = slice(row, row + rows)
        return nn(wk[...], gk_t[:, span]) + nn(wv[...], gv_t[:, span])

    final = q_reduces[1]
    if last > 0:
        final.step(0)
    back_out[:KVL, :] = project(0).astype(BF16)
    back_out[KVL:, :] = krope[:, :rows].astype(BF16)
    back = copy_of(back_out, back_in, b_send, b_recv, before)
    back.start()
    if last > 1:
        final.step(1)
    gkv_own[:KVL, :] = project(rows)
    gkv_own[KVL:, :] = krope[:, rows:]
    if last > 2:
        final.step(2)
    back.wait_recv()
    gkv_own[...] += back_in[...].astype(F32)
    for t in range(last):
        kv_reduce.step(t)
        if t + 3 < last:
            final.step(t + 3)

    for c in range(CHUNKS):
        q_reduces[c].total(stage_right)
        gq_ref[:, c * part_rows:(c + 1) * part_rows] = stage_right[...]
    kv_reduce.total(gkv_ref)

    kv_gather.finish()
    kv_reduce.finish()
    for c in range(CHUNKS):
        q_gathers[c].finish()
        q_reduces[c].finish()
    for i in range(n_head):
        copy_of(kv_ref, kv_prev.at[i], p_send.at[i], p_recv.at[i], after).wait_send()
    back.wait_send()


CHUNKS = 2
PIECE = 32


def on_device(n_ctx, n_head, q_latent, kv_latent, w_query, w_key, w_value, d_out):
    rows, q_cols = q_latent.shape
    kv_cols = kv_latent.shape[1]
    ql, qw = w_query.shape
    kw = w_key.shape[1]
    kvw = n_head * kv_cols
    heads = kw // NOPE
    part_rows = rows // CHUNKS
    vmem = pl.BlockSpec(memory_space=pltpu.VMEM)
    hbm = pl.BlockSpec(memory_space=pl.ANY)
    dma = pltpu.SemaphoreType.DMA
    some = (n_head,)
    each = (CHUNKS, n_head)
    out, gq_t, gkv_t = pl.pallas_call(
        functools.partial(kernel, n_ctx, n_head),
        out_shape=(
            jax.ShapeDtypeStruct((rows, kw), BF16),
            jax.ShapeDtypeStruct((q_cols, rows), F32),
            jax.ShapeDtypeStruct((kv_cols, rows), F32),
        ),
        in_specs=[vmem, vmem, vmem, hbm, hbm, hbm],
        out_specs=(vmem, vmem, vmem),
        scratch_shapes=[
            pltpu.VMEM((ql, qw), BF16),
            pltpu.VMEM((KVL, kw), BF16),
            pltpu.VMEM((KVL, kw), BF16),
            pltpu.VMEM((kw, KVL), BF16),
            pltpu.VMEM((kw, KVL), BF16),
            pltpu.VMEM((kw, rows), BF16),
            pltpu.VMEM((CHUNKS, n_head, part_rows, q_cols), BF16),
            pltpu.VMEM((n_head, kv_cols, rows), BF16),
            pltpu.VMEM((n_head, kv_cols, rows), BF16),
            pltpu.VMEM((kvw, 2 * rows), BF16),
            pltpu.VMEM((part_rows, qw), F32),
            pltpu.VMEM((rows, qw), BF16),
            pltpu.VMEM((kw, 2 * rows), BF16),
            pltpu.VMEM((kw, 2 * rows), BF16),
            pltpu.VMEM((part_rows, 2 * rows), F32),
            pltpu.VMEM((part_rows, 2 * rows), F32),
            pltpu.VMEM((part_rows, 2 * rows), F32),
            pltpu.VMEM((heads, rows, 2 * rows), BF16),
            pltpu.VMEM((heads, rows, 2 * rows), BF16),
            pltpu.VMEM((qw, rows), BF16),
            pltpu.VMEM((kw, 2 * rows), BF16),
            pltpu.VMEM((kw, 2 * rows), BF16),
            pltpu.VMEM((ROPE, 2 * rows), F32),
            pltpu.VMEM((kvw, rows), BF16),
            pltpu.VMEM((kvw, rows), BF16),
            pltpu.VMEM((CHUNKS, n_head, q_cols, part_rows), BF16),
            pltpu.VMEM((CHUNKS, n_head, q_cols, part_rows), BF16),
            pltpu.VMEM((CHUNKS, n_head, q_cols, part_rows), BF16),
            pltpu.VMEM((n_head, kv_cols, rows), BF16),
            pltpu.VMEM((n_head, kv_cols, rows), BF16),
            pltpu.VMEM((n_head, kv_cols, rows), BF16),
            pltpu.VMEM((kvw, rows), F32),
            pltpu.VMEM((q_cols, part_rows), F32),
            pltpu.VMEM((q_cols, part_rows), F32),
            pltpu.VMEM((part_rows, part_rows), F32),
            dma((3,)),
            dma(some), dma(some), dma(some),
            dma(each), dma(each), dma(each),
            dma(some), dma(some),
            dma, dma,
            dma(each), dma(each), dma(each),
            dma(some), dma(some), dma(some),
        ],
        compiler_params=pltpu.CompilerParams(
            collective_id=0, has_side_effects=True, vmem_limit_bytes=62 * 1024 * 1024,
        ),
        name="latent_attention",
    )(q_latent, kv_latent.T, d_out, w_query, w_key, w_value)
    return out, gq_t.T, gkv_t.T


def solution(mesh):
    return jax.shard_map(
        functools.partial(on_device, mesh.shape["ctx"], mesh.shape["head"]),
        mesh=mesh,
        in_specs=(
            P("ctx", "head"),
            P("ctx", "head"),
            P(None, "head"),
            P(None, "head"),
            P(None, "head"),
            P("ctx", "head"),
        ),
        out_specs=(P("ctx", "head"), P("ctx", "head"), P("ctx", "head")),
        check_vma=False,
    )
```

```python
import functools
import math

import jax
import jax.numpy as jnp
from jax import lax
from jax.experimental import pallas as pl
from jax.experimental.pallas import tpu as pltpu
from jax.sharding import PartitionSpec as P

KVL = 512
ROPE = 64
NOPE = 128
VDIM = 128
WIDTH = NOPE + ROPE
SCALE = WIDTH ** (-0.5)
F32 = jnp.float32
BF16 = jnp.bfloat16
MESH = pl.DeviceIdType.MESH


def nn(a, b):
    return jnp.dot(a, b, preferred_element_type=F32)


def nt(a, b):
    return lax.dot_general(a, b, (((1,), (1,)), ((), ())), preferred_element_type=F32)


def kernel(
    n_ctx, n_head,
    q_hbm, kv_hbm, do_hbm, wq_hbm, wk_hbm, wv_hbm,
    out_ref, gq_ref, gkv_ref,
    q_ref, kv_ref, do_ref, wq, wk, wv, wkt, wvt, dot_t, q_in, kv_in, kv_prev, lat_t, q_acc, q_b,
    keys_t, values_t, s_buf, dp_buf, p_buf, pb_all, ds_all, gq_t, gk_t, gv_t, krope, back_out, back_in,
    rq_out, rq_right, rq_left, rkv_out, rkv_right, rkv_left, gkv_own, stage_right, stage_left, stage_own,
    bias, w_sem, kv_r, kv_l, kv_recv, q_r, q_l, q_recv, p_send, p_recv,
    b_send, b_recv, rq_send, rq_rr, rq_rl, rkv_send, rkv_rr, rkv_rl,
):
    ctx = lax.axis_index("ctx")
    me = lax.axis_index("head")
    last = n_head - 1
    rows, q_cols = q_ref.shape
    part_rows = rows // CHUNKS
    kv_cols = kv_ref.shape[0]
    heads = wk.shape[1] // NOPE
    after = {"ctx": lax.rem(ctx + 1, n_ctx)}
    before = {"ctx": lax.rem(ctx + n_ctx - 1, n_ctx)}
    right = {"head": jnp.minimum(me + 1, last)}
    left = {"head": jnp.maximum(me - 1, 0)}
    has_right = me < last
    has_left = me > 0

    loads = [
        pltpu.make_async_copy(src, dst, w_sem.at[i])
        for i, (src, dst) in enumerate((
            (kv_hbm, kv_ref), (q_hbm, q_ref), (wk_hbm, wk), (wv_hbm, wv), (do_hbm, do_ref), (wq_hbm, wq),
        ))
    ]
    for load in loads:
        load.start()

    barrier = pltpu.get_barrier_semaphore()

    @pl.when(has_right)
    def _():
        pl.semaphore_signal(barrier, inc=1, device_id=right, device_id_type=MESH)

    @pl.when(has_left)
    def _():
        pl.semaphore_signal(barrier, inc=1, device_id=left, device_id_type=MESH)

    pl.semaphore_signal(barrier, inc=1, device_id=after, device_id_type=MESH)
    pl.semaphore_signal(barrier, inc=1, device_id=before, device_id_type=MESH)
    pl.semaphore_wait(barrier, 2 + jnp.minimum(me, 1) + jnp.minimum(last - me, 1))

    def copy_of(src, dst, send_sem, recv_sem, device):
        return pltpu.make_async_remote_copy(
            src_ref=src, dst_ref=dst, send_sem=send_sem, recv_sem=recv_sem,
            device_id=device, device_id_type=MESH,
        )

    class Gather:
        def __init__(self, own, slots, send_r, send_l, recv):
            self.own, self.slots, self.recv = own, slots, recv
            self.send_r, self.send_l = send_r, send_l

        def moves(self, t, act):
            @pl.when(has_right & (me >= t))
            def _():
                owner = me - t
                src = self.own if t == 0 else self.slots(owner)
                act(copy_of(src, self.slots(owner), self.send_r(t), self.recv(owner), right))

            @pl.when(has_left & (me + t <= last))
            def _():
                owner = me + t
                src = self.own if t == 0 else self.slots(owner)
                act(copy_of(src, self.slots(owner), self.send_l(t), self.recv(owner), left))

        def start(self, t):
            if t < last:
                self.moves(t, lambda copy: copy.start())

        def each(self, t, act):
            @pl.when(me - 1 - t >= 0)
            def _():
                act(me - 1 - t)

            @pl.when(me + 1 + t <= last)
            def _():
                act(me + 1 + t)

        def arrive(self, t, act=None):
            def wait(owner):
                slot = self.slots(owner)
                copy_of(slot, slot, self.send_r(0), self.recv(owner), right).wait_recv()
                if act is not None:
                    act(owner)

            self.each(t, wait)
            self.start(t + 1)

        def finish(self):
            for t in range(last):
                self.moves(t, lambda copy: copy.wait_send())

    def pass_on(owner, src):
        copy_of(src, kv_prev.at[owner], p_send.at[owner], p_recv.at[owner], after).start()

    kv_gather = Gather(kv_ref, lambda i: kv_in.at[i], lambda t: kv_r.at[t], lambda t: kv_l.at[t], lambda i: kv_recv.at[i])
    q_gathers = [
        Gather(
            q_ref.at[pl.ds(c * part_rows, part_rows), :],
            lambda i, c=c: q_in.at[c, i],
            lambda t, c=c: q_r.at[c, t],
            lambda t, c=c: q_l.at[c, t],
            lambda i, c=c: q_recv.at[c, i],
        )
        for c in range(CHUNKS)
    ]
    loads[0].wait()
    kv_gather.start(0)
    pass_on(me, kv_ref)
    loads[1].wait()
    q_gathers[0].start(0)
    kv_in[me] = kv_ref[...]
    for c in range(1, CHUNKS):
        q_in[c, me] = q_ref[c * part_rows:(c + 1) * part_rows, :]

    key_pos = lax.broadcasted_iota(jnp.int32, (part_rows, part_rows), 1)
    query_pos = lax.broadcasted_iota(jnp.int32, (part_rows, part_rows), 0)
    bias[...] = jnp.where(key_pos <= query_pos, F32(0.0), F32(-1e30))
    prev_mask = jnp.where(ctx == 0, F32(-1e30), F32(0.0))
    def clear_unseen():
        for c in range(CHUNKS - 1):
            seen = rows + (c + 1) * part_rows
            unseen = jnp.zeros((heads, part_rows, 2 * rows - seen), BF16)
            pb_all[:, c * part_rows:(c + 1) * part_rows, seen:] = unseen
            ds_all[:, c * part_rows:(c + 1) * part_rows, seen:] = unseen

    def turn(src, dst):
        @pl.loop(0, heads // 4)
        def _(j):
            for u in range(4):
                at = pl.multiple_of((4 * j + u) * NOPE, NOPE)
                dst[pl.ds(at, NOPE), :] = src[:, pl.ds(at, NOPE)].T

    def kv_step(t):
        kv_gather.arrive(t, lambda owner: pass_on(owner, kv_in.at[owner]))

    def q_step(c, t):
        q_gathers[c].arrive(t)

    def add_queries(c, block, owner, first=False):
        at = pl.multiple_of(owner * q_cols, q_cols)
        tile = 8 * WIDTH

        @pl.loop(0, wq.shape[1] // tile)
        def _(j):
            cols = pl.ds(pl.multiple_of(j * tile, tile), tile)
            part = nn(block[...], wq[pl.ds(at, q_cols), cols])
            if first:
                q_acc[:, cols] = part
            else:
                q_acc[:, cols] += part

    def own_queries(c):
        add_queries(c, q_ref.at[pl.ds(c * part_rows, part_rows), :], me, True)

    def add_arrived(c, t):
        q_gathers[c].each(t, lambda owner: add_queries(c, q_in.at[c, owner], owner))

    def finish_queries(c):
        q_b[c * part_rows:(c + 1) * part_rows, :] = q_acc[...].astype(BF16)

    def all_queries(c):
        tile = 4 * WIDTH

        @pl.loop(0, wq.shape[1] // tile)
        def _(j):
            cols = pl.ds(pl.multiple_of(j * tile, tile), tile)
            if q_cols % 128 == 0:
                total = nn(jnp.concatenate([q_in[c, i] for i in range(n_head)], 1), wq[:, cols])
            else:
                total = nn(q_in[c, 0], wq[:q_cols, cols])
                for i in range(1, n_head):
                    total += nn(q_in[c, i], wq[i * q_cols:(i + 1) * q_cols, cols])
            q_b[c * part_rows:(c + 1) * part_rows, cols] = total.astype(BF16)

    def assemble(parts, row):
        span = slice(row, row + rows)
        if kv_cols % 16 == 0:
            for i in range(n_head):
                lat_t[i * kv_cols:(i + 1) * kv_cols, span] = parts[i]
            return
        width = n_head * kv_cols
        total = None
        for i in range(n_head):
            dst = lax.broadcasted_iota(jnp.int32, (width, kv_cols), 0)
            src = lax.broadcasted_iota(jnp.int32, (width, kv_cols), 1) + i * kv_cols
            place = jnp.where(src == dst, F32(1.0), F32(0.0)).astype(BF16)
            term = nn(place, parts[i])
            total = term if total is None else total + term
        lat_t[:, span] = total.astype(BF16)

    def expand(row):
        tile = 4 * NOPE
        span = slice(row, row + rows)

        @pl.loop(0, heads // 4)
        def _(j):
            cols = pl.ds(pl.multiple_of(j * tile, tile), tile)
            main_t = lat_t[:KVL, span]
            keys_t[cols, span] = nn(wkt[cols, :], main_t).astype(BF16)
            values_t[cols, span] = nn(wvt[cols, :], main_t).astype(BF16)

    def window(h, odd):
        first = (h - 1 if odd else h) * WIDTH + (NOPE if odd else 0)
        return pl.ds(pl.multiple_of(first, NOPE), WIDTH + ROPE)

    def columns(h):
        return pl.ds(pl.multiple_of(h * NOPE, NOPE), NOPE)

    def seen_by(c):
        return rows + (c + 1) * part_rows

    def span_of(c):
        return slice(c * part_rows, (c + 1) * part_rows)

    def pieces(c):
        return [
            (slice(r, r + PIECE), slice(c * part_rows + r, c * part_rows + r + PIECE))
            for r in range(0, part_rows, PIECE)
        ]

    def score_stage(c, h, odd):
        seen = seen_by(c)
        query = q_b[span_of(c), window(h, odd)]
        key = [keys_t[columns(h), :seen], lat_t[KVL:, :seen]]
        pad = [jnp.zeros((ROPE, seen), BF16)]
        s_buf[odd, :, :seen] = nn(query, jnp.concatenate(pad + key if odd else key + pad, 0))

    def softmax_stage(c, h, odd):
        seen = seen_by(c)
        dp_buf[odd, :, :seen] = nn(do_ref[span_of(c), columns(h)], values_t[columns(h), :seen])
        for sub, row in pieces(c):
            scores = [s_buf[odd, sub, :rows] + prev_mask]
            if c > 0:
                scores.append(s_buf[odd, sub, rows:seen - part_rows])
            scores.append(s_buf[odd, sub, seen - part_rows:seen] + bias[sub, :])
            scores = jnp.concatenate(scores, 1)
            top = jnp.max(scores, 1, keepdims=True)
            expons = jnp.exp2((scores - top) * F32(SCALE * math.log2(math.e)))
            probs = expons * (F32(1.0) / jnp.sum(expons, 1, keepdims=True))
            p_buf[odd, sub, :seen] = probs
            pb_all[h, row, :seen] = probs.astype(BF16)

    def output_stage(c, h, odd):
        seen = seen_by(c)
        span = span_of(c)
        cols = columns(h)
        result = nt(pb_all[h, span, :seen], values_t[cols, :seen]).astype(BF16)
        out_ref[span, cols] = result
        row_dot = jnp.sum(do_ref[span, cols].astype(F32) * result.astype(F32), 1, keepdims=True)
        for sub, row in pieces(c):
            dscore = p_buf[odd, sub, :seen] * (dp_buf[odd, sub, :seen] - row_dot[sub]) * F32(SCALE)
            ds_all[h, row, :seen] = dscore.astype(BF16)

    def gradient_stage(c, h, odd, valid):
        seen = seen_by(c)
        span = span_of(c)
        cols = columns(h)
        key = jnp.concatenate([keys_t[cols, :seen], lat_t[KVL:, :seen]], 0)
        q_at = pl.ds(pl.multiple_of(h * WIDTH, ROPE), WIDTH)
        gq_t[q_at, span] = nt(key, ds_all[h, span, :seen]).astype(BF16)
        if c + 1 < CHUNKS:
            return
        query_t = q_b[:, window(h, odd)].T
        query_t = query_t[ROPE:] if odd else query_t[:WIDTH]
        g_key = nn(query_t, ds_all[h])
        gk_t[cols, :] = g_key[:NOPE].astype(BF16)
        g_rope = g_key[NOPE:].astype(BF16).astype(F32)
        krope[...] += g_rope if valid is None else jnp.where(valid, g_rope, F32(0.0))
        gv_t[cols, :] = nn(dot_t[cols, :], pb_all[h]).astype(BF16)

    def attention(c, hooks):
        trips = heads // 2
        count = len(hooks) + 1

        @pl.loop(0, trips)
        def _(t):
            for i, hook in enumerate(hooks):
                pl.when(t == trips * (i + 1) // count)(hook)
            for odd in range(2):
                gradient_stage(c, 2 * jnp.maximum(t - 3, 0) + odd, odd, t >= 3)
            for odd in range(2):
                output_stage(c, 2 * jnp.maximum(t - 2, 0) + odd, odd)
            for odd in range(2):
                softmax_stage(c, 2 * jnp.maximum(t - 1, 0) + odd, odd)
            for odd in range(2):
                score_stage(c, 2 * t + odd, odd)

        for t in range(trips, trips + 3):
            for odd in range(2):
                gradient_stage(c, 2 * (t - 3) + odd, odd, None)
            for odd in range(2):
                if t < trips + 2:
                    output_stage(c, 2 * (t - 2) + odd, odd)
            for odd in range(2):
                if t < trips + 1:
                    softmax_stage(c, 2 * (t - 1) + odd, odd)

    class Reduce:
        def __init__(self, part, out, in_right, in_left, send, recv_right, recv_left, stages):
            self.part, self.out, self.send = part, out, send
            self.ways = (
                (in_right, recv_right, right, stages[0], has_left),
                (in_left, recv_left, left, stages[1], has_right),
            )

        def step(self, tick):
            for way, (slots, recv, device, stage, joined) in enumerate(self.ways):
                lag = me if way == 0 else last - me
                owner = last - (tick - lag) if way == 0 else tick - lag

                @pl.when(tick >= lag)
                def _():
                    stage[...] = self.part(owner)

                    @pl.when(joined)
                    def _():
                        copy_of(slots(owner), slots(owner), self.send(owner), recv(owner), device).wait_recv()
                        stage[...] += slots(owner)[...].astype(F32)

                    self.out(owner)[...] = stage[...].astype(BF16)
                    copy_of(self.out(owner), slots(owner), self.send(owner), recv(owner), device).start()

        def total(self, stage, begin=True, end=True):
            if begin:
                stage[...] = self.part(me)
            if not end:
                return
            for slots, recv, device, _, joined in self.ways:
                @pl.when(joined)
                def _():
                    copy_of(slots(me), slots(me), self.send(me), recv(me), device).wait_recv()
                    stage[...] += slots(me)[...].astype(F32)

        def finish(self):
            for i in range(n_head):
                @pl.when(me != i)
                def _():
                    slot = self.out(i)
                    copy_of(slot, slot, self.send(i), self.send(i), right).wait_send()

    def query_part(c):
        def part(owner):
            at = pl.multiple_of(owner * q_cols, q_cols)
            return nn(wq[pl.ds(at, q_cols), :], gq_t[:, c * part_rows:(c + 1) * part_rows])

        return part

    def kv_part(owner):
        return gkv_own[pl.ds(pl.multiple_of(owner * kv_cols, 8), kv_cols), :]

    q_reduces = [
        Reduce(
            query_part(c),
            lambda i, c=c: rq_out.at[c, i],
            lambda i, c=c: rq_right.at[c, i],
            lambda i, c=c: rq_left.at[c, i],
            lambda i, c=c: rq_send.at[c, i],
            lambda i, c=c: rq_rr.at[c, i],
            lambda i, c=c: rq_rl.at[c, i],
            (stage_right, stage_left),
        )
        for c in range(CHUNKS)
    ]
    kv_stage = (gkv_ref, gkv_ref)
    kv_reduce = Reduce(
        kv_part,
        lambda i: rkv_out.at[i],
        lambda i: rkv_right.at[i],
        lambda i: rkv_left.at[i],
        lambda i: rkv_send.at[i],
        lambda i: rkv_rr.at[i],
        lambda i: rkv_rl.at[i],
        kv_stage,
    )

    loads[2].wait()
    turn(wk, wkt)
    if last > 0:
        kv_step(0)
    loads[3].wait()
    turn(wv, wvt)
    clear_unseen()
    loads[4].wait()
    turn(do_ref, dot_t)
    if last > 0:
        q_step(0, 0)
    loads[5].wait()
    own_queries(0)
    for t in range(1, last - 1):
        kv_step(t)
        add_arrived(0, t - 1)
        q_step(0, t)
    q_gathers[1].start(0)
    if last > 1:
        add_arrived(0, last - 2)
        kv_step(last - 1)
    assemble([kv_in[i] for i in range(n_head)], rows)
    expand(rows)
    if last > 1:
        q_step(0, last - 1)
    for i in range(n_head):
        copy_of(kv_ref, kv_prev.at[i], p_send.at[i], p_recv.at[i], after).wait_recv()
    assemble([kv_prev[i] for i in range(n_head)], 0)
    expand(0)
    if last > 0:
        add_arrived(0, last - 1)
    finish_queries(0)
    krope[...] = jnp.zeros_like(krope)
    if last > 0:
        q_step(1, 0)
    attention(0, [functools.partial(q_step, 1, t) for t in range(1, last)])
    if last > 0:
        q_reduces[0].step(0)
    all_queries(1)
    attention(1, [functools.partial(q_reduces[0].step, t) for t in range(1, last)])

    def project(row):
        span = slice(row, row + rows)
        return nn(wk[...], gk_t[:, span]) + nn(wv[...], gv_t[:, span])

    def finish_chunk(c, stage, begin=True):
        q_reduces[c].total(stage, begin)
        gq_ref[span_of(c), :] = stage[...].T

    final = q_reduces[1]
    if last > 0:
        final.step(0)
    back_out[:KVL, :] = project(0).astype(BF16)
    back_out[KVL:, :] = krope[:, :rows].astype(BF16)
    back = copy_of(back_out, back_in, b_send, b_recv, before)
    back.start()
    if last > 1:
        final.step(1)
    gkv_own[:KVL, :] = project(rows)
    gkv_own[KVL:, :] = krope[:, rows:]
    for t in range(2, last):
        final.step(t)
    back.wait_recv()
    gkv_own[...] += back_in[...].astype(F32)
    if last > 0:
        kv_reduce.step(0)
    finish_chunk(0, stage_own)
    if last > 1:
        kv_reduce.step(1)
    final.total(stage_own, end=False)
    for t in range(2, last):
        kv_reduce.step(t)
    finish_chunk(1, stage_own, False)
    kv_reduce.total(gkv_ref)

    kv_gather.finish()
    kv_reduce.finish()
    for c in range(CHUNKS):
        q_gathers[c].finish()
        q_reduces[c].finish()
    for i in range(n_head):
        copy_of(kv_ref, kv_prev.at[i], p_send.at[i], p_recv.at[i], after).wait_send()
    back.wait_send()


CHUNKS = 2
PIECE = 32


def store(*refs):
    sems = refs[6]
    copies = [pltpu.make_async_copy(refs[i], refs[i + 3], sems.at[i]) for i in range(3)]
    for copy in copies:
        copy.start()
    for copy in copies:
        copy.wait()


def on_device(n_ctx, n_head, q_latent, kv_latent, w_query, w_key, w_value, d_out):
    rows, q_cols = q_latent.shape
    kv_cols = kv_latent.shape[1]
    ql, qw = w_query.shape
    kw = w_key.shape[1]
    kvw = n_head * kv_cols
    heads = kw // NOPE
    part_rows = rows // CHUNKS
    vmem = pl.BlockSpec(memory_space=pltpu.VMEM)
    hbm = pl.BlockSpec(memory_space=pl.ANY)
    dma = pltpu.SemaphoreType.DMA
    some = (n_head,)
    each = (CHUNKS, n_head)
    results = (
        ((rows, kw), BF16),
        ((rows, q_cols), F32),
        ((kv_cols, rows), F32),
    )
    parts = pl.pallas_call(
        functools.partial(kernel, n_ctx, n_head),
        out_shape=tuple(pltpu.VMEM(shape, dtype) for shape, dtype in results),
        in_specs=[hbm] * 6,
        out_specs=(vmem, vmem, vmem),
        scratch_shapes=[
            pltpu.VMEM((rows, q_cols), BF16),
            pltpu.VMEM((kv_cols, rows), BF16),
            pltpu.VMEM((rows, kw), BF16),
            pltpu.VMEM((ql, qw), BF16),
            pltpu.VMEM((KVL, kw), BF16),
            pltpu.VMEM((KVL, kw), BF16),
            pltpu.VMEM((kw, KVL), BF16),
            pltpu.VMEM((kw, KVL), BF16),
            pltpu.VMEM((kw, rows), BF16),
            pltpu.VMEM((CHUNKS, n_head, part_rows, q_cols), BF16),
            pltpu.VMEM((n_head, kv_cols, rows), BF16),
            pltpu.VMEM((n_head, kv_cols, rows), BF16),
            pltpu.VMEM((kvw, 2 * rows), BF16),
            pltpu.VMEM((part_rows, qw), F32),
            pltpu.VMEM((rows, qw), BF16),
            pltpu.VMEM((kw, 2 * rows), BF16),
            pltpu.VMEM((kw, 2 * rows), BF16),
            pltpu.VMEM((2, part_rows, 2 * rows), F32),
            pltpu.VMEM((2, part_rows, 2 * rows), F32),
            pltpu.VMEM((2, part_rows, 2 * rows), F32),
            pltpu.VMEM((heads, rows, 2 * rows), BF16),
            pltpu.VMEM((heads, rows, 2 * rows), BF16),
            pltpu.VMEM((qw, rows), BF16),
            pltpu.VMEM((kw, 2 * rows), BF16),
            pltpu.VMEM((kw, 2 * rows), BF16),
            pltpu.VMEM((ROPE, 2 * rows), F32),
            pltpu.VMEM((kvw, rows), BF16),
            pltpu.VMEM((kvw, rows), BF16),
            pltpu.VMEM((CHUNKS, n_head, q_cols, part_rows), BF16),
            pltpu.VMEM((CHUNKS, n_head, q_cols, part_rows), BF16),
            pltpu.VMEM((CHUNKS, n_head, q_cols, part_rows), BF16),
            pltpu.VMEM((n_head, kv_cols, rows), BF16),
            pltpu.VMEM((n_head, kv_cols, rows), BF16),
            pltpu.VMEM((n_head, kv_cols, rows), BF16),
            pltpu.VMEM((kvw, rows), F32),
            pltpu.VMEM((q_cols, part_rows), F32),
            pltpu.VMEM((q_cols, part_rows), F32),
            pltpu.VMEM((q_cols, part_rows), F32),
            pltpu.VMEM((part_rows, part_rows), F32),
            dma((6,)),
            dma(some), dma(some), dma(some),
            dma(each), dma(each), dma(each),
            dma(some), dma(some),
            dma, dma,
            dma(each), dma(each), dma(each),
            dma(some), dma(some), dma(some),
        ],
        compiler_params=pltpu.CompilerParams(
            collective_id=0, has_side_effects=True, vmem_limit_bytes=58 * 1024 * 1024,
        ),
        name="latent_attention",
    )(q_latent, kv_latent.T, d_out, w_query, w_key, w_value)
    out, gq, gkv_t = pl.pallas_call(
        store,
        out_shape=tuple(jax.ShapeDtypeStruct(shape, dtype) for shape, dtype in results),
        in_specs=[vmem] * 3,
        out_specs=(hbm,) * 3,
        scratch_shapes=[dma((3,))],
        name="store_results",
    )(*(pltpu.with_memory_space_constraint(part, pltpu.VMEM) for part in parts))
    return out, gq, gkv_t.T


def solution(mesh):
    return jax.shard_map(
        functools.partial(on_device, mesh.shape["ctx"], mesh.shape["head"]),
        mesh=mesh,
        in_specs=(
            P("ctx", "head"),
            P("ctx", "head"),
            P(None, "head"),
            P(None, "head"),
            P(None, "head"),
            P("ctx", "head"),
        ),
        out_specs=(P("ctx", "head"), P("ctx", "head"), P("ctx", "head")),
        check_vma=False,
    )
```

```python
import functools
import math

import jax
import jax.numpy as jnp
from jax import lax
from jax.experimental import pallas as pl
from jax.experimental.pallas import tpu as pltpu
from jax.sharding import PartitionSpec as P

KVL = 512
ROPE = 64
NOPE = 128
VDIM = 128
WIDTH = NOPE + ROPE
SCALE = WIDTH ** (-0.5)
F32 = jnp.float32
BF16 = jnp.bfloat16
MESH = pl.DeviceIdType.MESH


def nn(a, b):
    return jnp.dot(a, b, preferred_element_type=F32)


def nt(a, b):
    return lax.dot_general(a, b, (((1,), (1,)), ((), ())), preferred_element_type=F32)


def kernel(
    n_ctx, n_head,
    q_hbm, kv_hbm, do_hbm, wq_hbm, wk_hbm, wv_hbm,
    out_ref, gq_ref, gkv_ref,
    q_ref, kv_ref, do_ref, wq, wk, wv, wkt, wvt, dot_t, q_in, kv_in, kv_prev, lat_t, q_acc, q_b,
    keys_t, values_t, s_buf, dp_buf, p_buf, pb_all, ds_all, gq_t, gk_t, gv_t, krope, back_out, back_in,
    rq_out, rq_right, rq_left, rkv_out, rkv_right, rkv_left, gkv_own, stage_right, stage_left, stage_own,
    bias, w_sem, kv_r, kv_l, kv_recv, q_r, q_l, q_recv, p_send, p_recv,
    b_send, b_recv, rq_send, rq_rr, rq_rl, rkv_send, rkv_rr, rkv_rl,
):
    ctx = lax.axis_index("ctx")
    me = lax.axis_index("head")
    last = n_head - 1
    rows, q_cols = q_ref.shape
    part_rows = rows // CHUNKS
    kv_cols = kv_ref.shape[0]
    heads = wk.shape[1] // NOPE
    after = {"ctx": lax.rem(ctx + 1, n_ctx)}
    before = {"ctx": lax.rem(ctx + n_ctx - 1, n_ctx)}
    right = {"head": jnp.minimum(me + 1, last)}
    left = {"head": jnp.maximum(me - 1, 0)}
    has_right = me < last
    has_left = me > 0

    loads = [
        pltpu.make_async_copy(src, dst, w_sem.at[i])
        for i, (src, dst) in enumerate((
            (kv_hbm, kv_ref), (q_hbm, q_ref), (wk_hbm, wk), (wv_hbm, wv), (do_hbm, do_ref), (wq_hbm, wq),
        ))
    ]
    for load in loads:
        load.start()

    barrier = pltpu.get_barrier_semaphore()

    @pl.when(has_right)
    def _():
        pl.semaphore_signal(barrier, inc=1, device_id=right, device_id_type=MESH)

    @pl.when(has_left)
    def _():
        pl.semaphore_signal(barrier, inc=1, device_id=left, device_id_type=MESH)

    pl.semaphore_signal(barrier, inc=1, device_id=after, device_id_type=MESH)
    pl.semaphore_signal(barrier, inc=1, device_id=before, device_id_type=MESH)
    pl.semaphore_wait(barrier, 2 + jnp.minimum(me, 1) + jnp.minimum(last - me, 1))

    def copy_of(src, dst, send_sem, recv_sem, device):
        return pltpu.make_async_remote_copy(
            src_ref=src, dst_ref=dst, send_sem=send_sem, recv_sem=recv_sem,
            device_id=device, device_id_type=MESH,
        )

    class Gather:
        def __init__(self, own, slots, send_r, send_l, recv):
            self.own, self.slots, self.recv = own, slots, recv
            self.send_r, self.send_l = send_r, send_l

        def moves(self, t, act):
            @pl.when(has_right & (me >= t))
            def _():
                owner = me - t
                src = self.own if t == 0 else self.slots(owner)
                act(copy_of(src, self.slots(owner), self.send_r(t), self.recv(owner), right))

            @pl.when(has_left & (me + t <= last))
            def _():
                owner = me + t
                src = self.own if t == 0 else self.slots(owner)
                act(copy_of(src, self.slots(owner), self.send_l(t), self.recv(owner), left))

        def start(self, t):
            if t < last:
                self.moves(t, lambda copy: copy.start())

        def each(self, t, act):
            @pl.when(me - 1 - t >= 0)
            def _():
                act(me - 1 - t)

            @pl.when(me + 1 + t <= last)
            def _():
                act(me + 1 + t)

        def arrive(self, t, act=None):
            def wait(owner):
                slot = self.slots(owner)
                copy_of(slot, slot, self.send_r(0), self.recv(owner), right).wait_recv()
                if act is not None:
                    act(owner)

            self.each(t, wait)
            self.start(t + 1)

        def finish(self):
            for t in range(last):
                self.moves(t, lambda copy: copy.wait_send())

    def pass_on(owner, src):
        copy_of(src, kv_prev.at[owner], p_send.at[owner], p_recv.at[owner], after).start()

    kv_gather = Gather(kv_ref, lambda i: kv_in.at[i], lambda t: kv_r.at[t], lambda t: kv_l.at[t], lambda i: kv_recv.at[i])
    q_gathers = [
        Gather(
            q_ref.at[pl.ds(c * part_rows, part_rows), :],
            lambda i, c=c: q_in.at[c, i],
            lambda t, c=c: q_r.at[c, t],
            lambda t, c=c: q_l.at[c, t],
            lambda i, c=c: q_recv.at[c, i],
        )
        for c in range(CHUNKS)
    ]
    loads[0].wait()
    kv_gather.start(0)
    pass_on(me, kv_ref)
    loads[1].wait()
    q_gathers[0].start(0)
    kv_in[me] = kv_ref[...]
    for c in range(1, CHUNKS):
        q_in[c, me] = q_ref[c * part_rows:(c + 1) * part_rows, :]

    key_pos = lax.broadcasted_iota(jnp.int32, (part_rows, part_rows), 1)
    query_pos = lax.broadcasted_iota(jnp.int32, (part_rows, part_rows), 0)
    bias[...] = jnp.where(key_pos <= query_pos, F32(0.0), F32(-1e30))
    prev_mask = jnp.where(ctx == 0, F32(-1e30), F32(0.0))
    def clear_unseen():
        for c in range(CHUNKS - 1):
            seen = rows + (c + 1) * part_rows
            unseen = jnp.zeros((heads, part_rows, 2 * rows - seen), BF16)
            pb_all[:, c * part_rows:(c + 1) * part_rows, seen:] = unseen
            ds_all[:, c * part_rows:(c + 1) * part_rows, seen:] = unseen

    def turn(src, dst):
        @pl.loop(0, heads // 4)
        def _(j):
            for u in range(4):
                at = pl.multiple_of((4 * j + u) * NOPE, NOPE)
                dst[pl.ds(at, NOPE), :] = src[:, pl.ds(at, NOPE)].T

    def kv_step(t):
        kv_gather.arrive(t, lambda owner: pass_on(owner, kv_in.at[owner]))

    def q_step(c, t):
        q_gathers[c].arrive(t)

    def add_queries(c, block, owner, first=False):
        at = pl.multiple_of(owner * q_cols, q_cols)
        tile = heads * WIDTH

        @pl.loop(0, wq.shape[1] // tile)
        def _(j):
            cols = pl.ds(pl.multiple_of(j * tile, tile), tile)
            part = nn(block[...], wq[pl.ds(at, q_cols), cols])
            if first:
                q_acc[:, cols] = part
            else:
                q_acc[:, cols] += part

    def own_queries(c):
        add_queries(c, q_ref.at[pl.ds(c * part_rows, part_rows), :], me, True)

    def add_arrived(c, t):
        q_gathers[c].each(t, lambda owner: add_queries(c, q_in.at[c, owner], owner))

    def finish_queries(c):
        q_b[c * part_rows:(c + 1) * part_rows, :] = q_acc[...].astype(BF16)

    def all_queries(c):
        tile = 8 * WIDTH

        @pl.loop(0, wq.shape[1] // tile)
        def _(j):
            cols = pl.ds(pl.multiple_of(j * tile, tile), tile)
            if q_cols % 128 == 0:
                total = nn(jnp.concatenate([q_in[c, i] for i in range(n_head)], 1), wq[:, cols])
            else:
                total = nn(q_in[c, 0], wq[:q_cols, cols])
                for i in range(1, n_head):
                    total += nn(q_in[c, i], wq[i * q_cols:(i + 1) * q_cols, cols])
            q_b[c * part_rows:(c + 1) * part_rows, cols] = total.astype(BF16)

    def assemble(parts, row):
        span = slice(row, row + rows)
        if kv_cols % 16 == 0:
            for i in range(n_head):
                lat_t[i * kv_cols:(i + 1) * kv_cols, span] = parts[i]
            return
        width = n_head * kv_cols
        total = None
        for i in range(n_head):
            dst = lax.broadcasted_iota(jnp.int32, (width, kv_cols), 0)
            src = lax.broadcasted_iota(jnp.int32, (width, kv_cols), 1) + i * kv_cols
            place = jnp.where(src == dst, F32(1.0), F32(0.0)).astype(BF16)
            term = nn(place, parts[i])
            total = term if total is None else total + term
        lat_t[:, span] = total.astype(BF16)

    def expand(row):
        tile = 8 * NOPE
        span = slice(row, row + rows)

        @pl.loop(0, heads // 8)
        def _(j):
            cols = pl.ds(pl.multiple_of(j * tile, tile), tile)
            main_t = lat_t[:KVL, span]
            keys_t[cols, span] = nn(wkt[cols, :], main_t).astype(BF16)
            values_t[cols, span] = nn(wvt[cols, :], main_t).astype(BF16)

    def window(h, odd):
        first = (h - 1 if odd else h) * WIDTH + (NOPE if odd else 0)
        return pl.ds(pl.multiple_of(first, NOPE), WIDTH + ROPE)

    def columns(h):
        return pl.ds(pl.multiple_of(h * NOPE, NOPE), NOPE)

    def seen_by(c):
        return rows + (c + 1) * part_rows

    def span_of(c):
        return slice(c * part_rows, (c + 1) * part_rows)

    def pieces(c):
        return [
            (slice(r, r + PIECE), slice(c * part_rows + r, c * part_rows + r + PIECE))
            for r in range(0, part_rows, PIECE)
        ]

    def score_stage(c, h, odd):
        seen = seen_by(c)
        query = q_b[span_of(c), window(h, odd)]
        key = [keys_t[columns(h), :seen], lat_t[KVL:, :seen]]
        pad = [jnp.zeros((ROPE, seen), BF16)]
        s_buf[odd, :, :seen] = nn(query, jnp.concatenate(pad + key if odd else key + pad, 0))

    def softmax_stage(c, h, odd):
        seen = seen_by(c)
        dp_buf[odd, :, :seen] = nn(do_ref[span_of(c), columns(h)], values_t[columns(h), :seen])
        for sub, row in pieces(c):
            scores = [s_buf[odd, sub, :rows] + prev_mask]
            if c > 0:
                scores.append(s_buf[odd, sub, rows:seen - part_rows])
            scores.append(s_buf[odd, sub, seen - part_rows:seen] + bias[sub, :])
            scores = jnp.concatenate(scores, 1)
            top = jnp.max(scores, 1, keepdims=True)
            expons = jnp.exp2((scores - top) * F32(SCALE * math.log2(math.e)))
            probs = expons * (F32(1.0) / jnp.sum(expons, 1, keepdims=True))
            p_buf[odd, sub, :seen] = probs
            pb_all[h, row, :seen] = probs.astype(BF16)

    def output_stage(c, h, odd):
        seen = seen_by(c)
        span = span_of(c)
        cols = columns(h)
        result = nt(pb_all[h, span, :seen], values_t[cols, :seen]).astype(BF16)
        out_ref[span, cols] = result
        row_dot = jnp.sum(do_ref[span, cols].astype(F32) * result.astype(F32), 1, keepdims=True)
        for sub, row in pieces(c):
            dscore = p_buf[odd, sub, :seen] * (dp_buf[odd, sub, :seen] - row_dot[sub]) * F32(SCALE)
            ds_all[h, row, :seen] = dscore.astype(BF16)

    def gradient_stage(c, h, odd):
        seen = seen_by(c)
        span = span_of(c)
        cols = columns(h)
        key = jnp.concatenate([keys_t[cols, :seen], lat_t[KVL:, :seen]], 0)
        q_at = pl.ds(pl.multiple_of(h * WIDTH, ROPE), WIDTH)
        gq_t[q_at, span] = nt(key, ds_all[h, span, :seen]).astype(BF16)
        if c + 1 < CHUNKS:
            return
        query_t = q_b[:, window(h, odd)].T
        query_t = query_t[ROPE:] if odd else query_t[:WIDTH]
        g_key = nn(query_t, ds_all[h])
        gk_t[cols, :] = g_key[:NOPE].astype(BF16)
        krope[...] += g_key[NOPE:].astype(BF16).astype(F32)
        gv_t[cols, :] = nn(dot_t[cols, :], pb_all[h]).astype(BF16)

    def attention(c, hooks):
        trips = heads // 2

        def trip(t, stages):
            if "g" in stages:
                for odd in range(2):
                    gradient_stage(c, 2 * (t - 3) + odd, odd)
            if "o" in stages:
                for odd in range(2):
                    output_stage(c, 2 * (t - 2) + odd, odd)
            if "p" in stages:
                for odd in range(2):
                    softmax_stage(c, 2 * (t - 1) + odd, odd)
            if "s" in stages:
                for odd in range(2):
                    score_stage(c, 2 * t + odd, odd)

        trip(0, "s")
        trip(1, "ps")
        trip(2, "ops")

        @pl.loop(3, trips)
        def _(t):
            for i, hook in enumerate(hooks):
                pl.when(t == 3 + ((trips - 3) * (2 * i + 1)) // (2 * len(hooks)))(hook)
            trip(t, "gops")

        trip(trips, "gop")
        trip(trips + 1, "go")
        trip(trips + 2, "g")

    class Reduce:
        def __init__(self, part, out, in_right, in_left, send, recv_right, recv_left, stages):
            self.part, self.out, self.send = part, out, send
            self.ways = (
                (in_right, recv_right, right, stages[0], has_left),
                (in_left, recv_left, left, stages[1], has_right),
            )

        def step(self, tick):
            for way, (slots, recv, device, stage, joined) in enumerate(self.ways):
                lag = me if way == 0 else last - me
                owner = last - (tick - lag) if way == 0 else tick - lag

                @pl.when(tick >= lag)
                def _():
                    stage[...] = self.part(owner)

                    @pl.when(joined)
                    def _():
                        copy_of(slots(owner), slots(owner), self.send(owner), recv(owner), device).wait_recv()
                        stage[...] += slots(owner)[...].astype(F32)

                    self.out(owner)[...] = stage[...].astype(BF16)
                    copy_of(self.out(owner), slots(owner), self.send(owner), recv(owner), device).start()

        def total(self, stage, begin=True, end=True):
            if begin:
                stage[...] = self.part(me)
            if not end:
                return
            for slots, recv, device, _, joined in self.ways:
                @pl.when(joined)
                def _():
                    copy_of(slots(me), slots(me), self.send(me), recv(me), device).wait_recv()
                    stage[...] += slots(me)[...].astype(F32)

        def finish(self):
            for i in range(n_head):
                @pl.when(me != i)
                def _():
                    slot = self.out(i)
                    copy_of(slot, slot, self.send(i), self.send(i), right).wait_send()

    def query_part(c):
        def part(owner):
            at = pl.multiple_of(owner * q_cols, q_cols)
            return nn(wq[pl.ds(at, q_cols), :], gq_t[:, c * part_rows:(c + 1) * part_rows])

        return part

    def kv_part(c):
        def part(owner):
            return gkv_own[pl.ds(pl.multiple_of(owner * kv_cols, 8), kv_cols), span_of(c)]

        return part

    q_reduces = [
        Reduce(
            query_part(c),
            lambda i, c=c: rq_out.at[c, i],
            lambda i, c=c: rq_right.at[c, i],
            lambda i, c=c: rq_left.at[c, i],
            lambda i, c=c: rq_send.at[c, i],
            lambda i, c=c: rq_rr.at[c, i],
            lambda i, c=c: rq_rl.at[c, i],
            (stage_right, stage_left),
        )
        for c in range(CHUNKS)
    ]
    kv_reduces = [
        Reduce(
            kv_part(c),
            lambda i, c=c: rkv_out.at[c, i],
            lambda i, c=c: rkv_right.at[c, i],
            lambda i, c=c: rkv_left.at[c, i],
            lambda i, c=c: rkv_send.at[c, i],
            lambda i, c=c: rkv_rr.at[c, i],
            lambda i, c=c: rkv_rl.at[c, i],
            (gkv_ref.at[:, span_of(c)],) * 2,
        )
        for c in range(CHUNKS)
    ]

    loads[2].wait()
    turn(wk, wkt)
    if last > 0:
        kv_step(0)
    loads[3].wait()
    turn(wv, wvt)
    clear_unseen()
    krope[...] = jnp.zeros_like(krope)
    loads[4].wait()
    turn(do_ref, dot_t)
    if last > 0:
        q_step(0, 0)
    loads[5].wait()
    own_queries(0)
    for t in range(1, last - 1):
        kv_step(t)
        add_arrived(0, t - 1)
        q_step(0, t)
    q_gathers[1].start(0)
    if last > 1:
        add_arrived(0, last - 2)
        kv_step(last - 1)
    assemble([kv_in[i] for i in range(n_head)], rows)
    expand(rows)
    if last > 1:
        q_step(0, last - 1)
    for i in range(n_head):
        copy_of(kv_ref, kv_prev.at[i], p_send.at[i], p_recv.at[i], after).wait_recv()
    assemble([kv_prev[i] for i in range(n_head)], 0)
    expand(0)
    if last > 0:
        q_step(1, 0)
        add_arrived(0, last - 1)
    finish_queries(0)
    attention(0, [functools.partial(q_step, 1, t) for t in range(1, last - 1)])
    if last > 0:
        q_reduces[0].step(0)
    if last > 1:
        q_step(1, last - 1)
    all_queries(1)
    attention(1, [functools.partial(q_reduces[0].step, t) for t in range(1, last)])

    def project(row):
        span = slice(row, row + rows)
        return nn(wk[...], gk_t[:, span]) + nn(wv[...], gv_t[:, span])

    def finish_chunk(c, stage, begin=True):
        q_reduces[c].total(stage, begin)
        gq_ref[span_of(c), :] = stage[...].T

    final = q_reduces[1]
    if last > 0:
        final.step(0)
    back_out[:KVL, :] = project(0).astype(BF16)
    back_out[KVL:, :] = krope[:, :rows].astype(BF16)
    back = copy_of(back_out, back_in, b_send, b_recv, before)
    back.start()
    if last > 1:
        final.step(1)
    gkv_own[:KVL, :] = project(rows)
    gkv_own[KVL:, :] = krope[:, rows:]
    for t in range(2, last):
        final.step(t)
    finish_chunk(0, stage_own)
    final.total(stage_own, end=False)
    back.wait_recv()
    gkv_own[...] += back_in[...].astype(F32)
    for t in range(last):
        for c in range(CHUNKS):
            kv_reduces[c].step(t)
    finish_chunk(1, stage_own, False)
    for c in range(CHUNKS):
        kv_reduces[c].total(gkv_ref.at[:, span_of(c)])

    kv_gather.finish()
    for c in range(CHUNKS):
        kv_reduces[c].finish()
        q_gathers[c].finish()
        q_reduces[c].finish()
    for i in range(n_head):
        copy_of(kv_ref, kv_prev.at[i], p_send.at[i], p_recv.at[i], after).wait_send()
    back.wait_send()


CHUNKS = 2
PIECE = 32


def store(*refs):
    sems = refs[6]
    copies = [pltpu.make_async_copy(refs[i], refs[i + 3], sems.at[i]) for i in range(3)]
    for copy in copies:
        copy.start()
    for copy in copies:
        copy.wait()


def on_device(n_ctx, n_head, q_latent, kv_latent, w_query, w_key, w_value, d_out):
    rows, q_cols = q_latent.shape
    kv_cols = kv_latent.shape[1]
    ql, qw = w_query.shape
    kw = w_key.shape[1]
    kvw = n_head * kv_cols
    heads = kw // NOPE
    part_rows = rows // CHUNKS
    vmem = pl.BlockSpec(memory_space=pltpu.VMEM)
    hbm = pl.BlockSpec(memory_space=pl.ANY)
    dma = pltpu.SemaphoreType.DMA
    some = (n_head,)
    each = (CHUNKS, n_head)
    results = (
        ((rows, kw), BF16),
        ((rows, q_cols), F32),
        ((kv_cols, rows), F32),
    )
    parts = pl.pallas_call(
        functools.partial(kernel, n_ctx, n_head),
        out_shape=tuple(pltpu.VMEM(shape, dtype) for shape, dtype in results),
        in_specs=[hbm] * 6,
        out_specs=(vmem, vmem, vmem),
        scratch_shapes=[
            pltpu.VMEM((rows, q_cols), BF16),
            pltpu.VMEM((kv_cols, rows), BF16),
            pltpu.VMEM((rows, kw), BF16),
            pltpu.VMEM((ql, qw), BF16),
            pltpu.VMEM((KVL, kw), BF16),
            pltpu.VMEM((KVL, kw), BF16),
            pltpu.VMEM((kw, KVL), BF16),
            pltpu.VMEM((kw, KVL), BF16),
            pltpu.VMEM((kw, rows), BF16),
            pltpu.VMEM((CHUNKS, n_head, part_rows, q_cols), BF16),
            pltpu.VMEM((n_head, kv_cols, rows), BF16),
            pltpu.VMEM((n_head, kv_cols, rows), BF16),
            pltpu.VMEM((kvw, 2 * rows), BF16),
            pltpu.VMEM((part_rows, qw), F32),
            pltpu.VMEM((rows, qw), BF16),
            pltpu.VMEM((kw, 2 * rows), BF16),
            pltpu.VMEM((kw, 2 * rows), BF16),
            pltpu.VMEM((2, part_rows, 2 * rows), F32),
            pltpu.VMEM((2, part_rows, 2 * rows), F32),
            pltpu.VMEM((2, part_rows, 2 * rows), F32),
            pltpu.VMEM((heads, rows, 2 * rows), BF16),
            pltpu.VMEM((heads, rows, 2 * rows), BF16),
            pltpu.VMEM((qw, rows), BF16),
            pltpu.VMEM((kw, 2 * rows), BF16),
            pltpu.VMEM((kw, 2 * rows), BF16),
            pltpu.VMEM((ROPE, 2 * rows), F32),
            pltpu.VMEM((kvw, rows), BF16),
            pltpu.VMEM((kvw, rows), BF16),
            pltpu.VMEM((CHUNKS, n_head, q_cols, part_rows), BF16),
            pltpu.VMEM((CHUNKS, n_head, q_cols, part_rows), BF16),
            pltpu.VMEM((CHUNKS, n_head, q_cols, part_rows), BF16),
            pltpu.VMEM((CHUNKS, n_head, kv_cols, part_rows), BF16),
            pltpu.VMEM((CHUNKS, n_head, kv_cols, part_rows), BF16),
            pltpu.VMEM((CHUNKS, n_head, kv_cols, part_rows), BF16),
            pltpu.VMEM((kvw, rows), F32),
            pltpu.VMEM((q_cols, part_rows), F32),
            pltpu.VMEM((q_cols, part_rows), F32),
            pltpu.VMEM((q_cols, part_rows), F32),
            pltpu.VMEM((part_rows, part_rows), F32),
            dma((6,)),
            dma(some), dma(some), dma(some),
            dma(each), dma(each), dma(each),
            dma(some), dma(some),
            dma, dma,
            dma(each), dma(each), dma(each),
            dma(each), dma(each), dma(each),
        ],
        compiler_params=pltpu.CompilerParams(
            collective_id=0, has_side_effects=True, vmem_limit_bytes=58 * 1024 * 1024,
        ),
        name="latent_attention",
    )(q_latent, kv_latent.T, d_out, w_query, w_key, w_value)
    out, gq, gkv_t = pl.pallas_call(
        store,
        out_shape=tuple(jax.ShapeDtypeStruct(shape, dtype) for shape, dtype in results),
        in_specs=[vmem] * 3,
        out_specs=(hbm,) * 3,
        scratch_shapes=[dma((3,))],
        name="store_results",
    )(*(pltpu.with_memory_space_constraint(part, pltpu.VMEM) for part in parts))
    return out, gq, gkv_t.T


def solution(mesh):
    return jax.shard_map(
        functools.partial(on_device, mesh.shape["ctx"], mesh.shape["head"]),
        mesh=mesh,
        in_specs=(
            P("ctx", "head"),
            P("ctx", "head"),
            P(None, "head"),
            P(None, "head"),
            P(None, "head"),
            P("ctx", "head"),
        ),
        out_specs=(P("ctx", "head"), P("ctx", "head"), P("ctx", "head")),
        check_vma=False,
    )
```

```python
import functools
import math

import jax
import jax.numpy as jnp
from jax import lax
from jax.experimental import pallas as pl
from jax.experimental.pallas import tpu as pltpu
from jax.sharding import PartitionSpec as P

KVL = 512
ROPE = 64
NOPE = 128
VDIM = 128
WIDTH = NOPE + ROPE
SCALE = WIDTH ** (-0.5)
F32 = jnp.float32
BF16 = jnp.bfloat16
MESH = pl.DeviceIdType.MESH


def nn(a, b):
    return jnp.dot(a, b, preferred_element_type=F32)


def nt(a, b):
    return lax.dot_general(a, b, (((1,), (1,)), ((), ())), preferred_element_type=F32)


def kernel(
    n_ctx, n_head,
    q_hbm, kv_hbm, do_hbm, wq_hbm, wk_hbm, wv_hbm,
    out_ref, gq_ref, gkv_ref,
    q_ref, kv_ref, do_ref, wq, wk, wv, wkt, wvt, dot_t, q_in, kv_in, kv_prev, lat_t, q_acc, q_b,
    keys_t, values_t, s_buf, dp_buf, p_buf, pb_all, ds_all, gq_t, gk_t, gv_t, krope, back_out, back_in,
    rq_out, rq_right, rq_left, rkv_out, rkv_right, rkv_left, gkv_own, stage_right, stage_own,
    bias, w_sem, kv_r, kv_l, kv_recv, q_r, q_l, q_recv, p_send, p_recv,
    b_send, b_recv, rq_send, rq_rr, rq_rl, rkv_send, rkv_rr, rkv_rl,
):
    ctx = lax.axis_index("ctx")
    me = lax.axis_index("head")
    last = n_head - 1
    rows, q_cols = q_ref.shape
    part_rows = rows // CHUNKS
    kv_cols = kv_ref.shape[0]
    heads = wk.shape[1] // NOPE
    after = {"ctx": lax.rem(ctx + 1, n_ctx)}
    before = {"ctx": lax.rem(ctx + n_ctx - 1, n_ctx)}
    right = {"head": jnp.minimum(me + 1, last)}
    left = {"head": jnp.maximum(me - 1, 0)}
    has_right = me < last
    has_left = me > 0

    loads = [
        pltpu.make_async_copy(src, dst, w_sem.at[i])
        for i, (src, dst) in enumerate((
            (kv_hbm, kv_ref), (q_hbm, q_ref), (wk_hbm, wk), (wv_hbm, wv), (do_hbm, do_ref), (wq_hbm, wq),
        ))
    ]
    for load in loads:
        load.start()

    barrier = pltpu.get_barrier_semaphore()

    for peer in range(n_head):
        @pl.when(me != peer)
        def _():
            pl.semaphore_signal(barrier, inc=1, device_id={"head": peer}, device_id_type=MESH)

    pl.semaphore_signal(barrier, inc=1, device_id=after, device_id_type=MESH)
    pl.semaphore_signal(barrier, inc=1, device_id=before, device_id_type=MESH)
    pl.semaphore_wait(barrier, 2 + last)

    def copy_of(src, dst, send_sem, recv_sem, device):
        return pltpu.make_async_remote_copy(
            src_ref=src, dst_ref=dst, send_sem=send_sem, recv_sem=recv_sem,
            device_id=device, device_id_type=MESH,
        )

    class Gather:
        def __init__(self, own, slots, send_r, send_l, recv):
            self.own, self.slots, self.recv = own, slots, recv
            self.send_r, self.send_l = send_r, send_l

        def moves(self, t, act):
            @pl.when(has_right & (me >= t))
            def _():
                owner = me - t
                src = self.own if t == 0 else self.slots(owner)
                act(copy_of(src, self.slots(owner), self.send_r(t), self.recv(owner), right))

            @pl.when(has_left & (me + t <= last))
            def _():
                owner = me + t
                src = self.own if t == 0 else self.slots(owner)
                act(copy_of(src, self.slots(owner), self.send_l(t), self.recv(owner), left))

        def start(self, t):
            if t < last:
                self.moves(t, lambda copy: copy.start())

        def each(self, t, act):
            @pl.when(me - 1 - t >= 0)
            def _():
                act(me - 1 - t)

            @pl.when(me + 1 + t <= last)
            def _():
                act(me + 1 + t)

        def arrive(self, t, act=None):
            def wait(owner):
                slot = self.slots(owner)
                copy_of(slot, slot, self.send_r(0), self.recv(owner), right).wait_recv()
                if act is not None:
                    act(owner)

            self.each(t, wait)
            self.start(t + 1)

        def finish(self):
            for t in range(last):
                self.moves(t, lambda copy: copy.wait_send())

    def pass_on(owner, src):
        copy_of(src, kv_prev.at[owner], p_send.at[owner], p_recv.at[owner], after).start()

    kv_gather = Gather(kv_ref, lambda i: kv_in.at[i], lambda t: kv_r.at[t], lambda t: kv_l.at[t], lambda i: kv_recv.at[i])
    q_gathers = [
        Gather(
            q_ref.at[pl.ds(c * part_rows, part_rows), :],
            lambda i, c=c: q_in.at[c, i],
            lambda t, c=c: q_r.at[c, t],
            lambda t, c=c: q_l.at[c, t],
            lambda i, c=c: q_recv.at[c, i],
        )
        for c in range(CHUNKS)
    ]
    loads[0].wait()
    kv_gather.start(0)
    pass_on(me, kv_ref)
    loads[1].wait()
    q_gathers[0].start(0)
    kv_in[me] = kv_ref[...]
    for c in range(1, CHUNKS):
        q_in[c, me] = q_ref[c * part_rows:(c + 1) * part_rows, :]

    key_pos = lax.broadcasted_iota(jnp.int32, (part_rows, part_rows), 1)
    query_pos = lax.broadcasted_iota(jnp.int32, (part_rows, part_rows), 0)
    bias[...] = jnp.where(key_pos <= query_pos, F32(0.0), F32(-1e30))
    prev_mask = jnp.where(ctx == 0, F32(-1e30), F32(0.0))
    def clear_unseen():
        for c in range(CHUNKS - 1):
            seen = rows + (c + 1) * part_rows
            unseen = jnp.zeros((heads, part_rows, 2 * rows - seen), BF16)
            pb_all[:, c * part_rows:(c + 1) * part_rows, seen:] = unseen
            ds_all[:, c * part_rows:(c + 1) * part_rows, seen:] = unseen

    def turn(src, dst):
        @pl.loop(0, heads // 4)
        def _(j):
            for u in range(4):
                at = pl.multiple_of((4 * j + u) * NOPE, NOPE)
                dst[pl.ds(at, NOPE), :] = src[:, pl.ds(at, NOPE)].T

    def kv_step(t):
        kv_gather.arrive(t, lambda owner: pass_on(owner, kv_in.at[owner]))

    def q_step(c, t):
        q_gathers[c].arrive(t)

    def add_queries(c, block, owner, first=False):
        at = pl.multiple_of(owner * q_cols, q_cols)
        tile = heads * WIDTH

        @pl.loop(0, wq.shape[1] // tile)
        def _(j):
            cols = pl.ds(pl.multiple_of(j * tile, tile), tile)
            part = nn(block[...], wq[pl.ds(at, q_cols), cols])
            if first:
                q_acc[:, cols] = part
            else:
                q_acc[:, cols] += part

    def own_queries(c):
        add_queries(c, q_ref.at[pl.ds(c * part_rows, part_rows), :], me, True)

    def add_arrived(c, t):
        q_gathers[c].each(t, lambda owner: add_queries(c, q_in.at[c, owner], owner))

    def finish_queries(c):
        q_b[c * part_rows:(c + 1) * part_rows, :] = q_acc[...].astype(BF16)

    def all_queries(c):
        tile = 8 * WIDTH

        @pl.loop(0, wq.shape[1] // tile)
        def _(j):
            cols = pl.ds(pl.multiple_of(j * tile, tile), tile)
            if q_cols % 128 == 0:
                total = nn(jnp.concatenate([q_in[c, i] for i in range(n_head)], 1), wq[:, cols])
            else:
                total = nn(q_in[c, 0], wq[:q_cols, cols])
                for i in range(1, n_head):
                    total += nn(q_in[c, i], wq[i * q_cols:(i + 1) * q_cols, cols])
            q_b[c * part_rows:(c + 1) * part_rows, cols] = total.astype(BF16)

    def assemble(parts, row):
        span = slice(row, row + rows)
        if kv_cols % 16 == 0:
            for i in range(n_head):
                lat_t[i * kv_cols:(i + 1) * kv_cols, span] = parts[i]
            return
        width = n_head * kv_cols
        total = None
        for i in range(n_head):
            dst = lax.broadcasted_iota(jnp.int32, (width, kv_cols), 0)
            src = lax.broadcasted_iota(jnp.int32, (width, kv_cols), 1) + i * kv_cols
            place = jnp.where(src == dst, F32(1.0), F32(0.0)).astype(BF16)
            term = nn(place, parts[i])
            total = term if total is None else total + term
        lat_t[:, span] = total.astype(BF16)

    def expand(row):
        tile = 8 * NOPE
        span = slice(row, row + rows)

        @pl.loop(0, heads // 8)
        def _(j):
            cols = pl.ds(pl.multiple_of(j * tile, tile), tile)
            main_t = lat_t[:KVL, span]
            keys_t[cols, span] = nn(wkt[cols, :], main_t).astype(BF16)
            values_t[cols, span] = nn(wvt[cols, :], main_t).astype(BF16)

    def window(h, odd):
        first = (h - 1 if odd else h) * WIDTH + (NOPE if odd else 0)
        return pl.ds(pl.multiple_of(first, NOPE), WIDTH + ROPE)

    def columns(h):
        return pl.ds(pl.multiple_of(h * NOPE, NOPE), NOPE)

    def seen_by(c):
        return rows + (c + 1) * part_rows

    def span_of(c):
        return slice(c * part_rows, (c + 1) * part_rows)

    def pieces(c):
        return [
            (slice(r, r + PIECE), slice(c * part_rows + r, c * part_rows + r + PIECE))
            for r in range(0, part_rows, PIECE)
        ]

    def score_stage(c, h, odd):
        seen = seen_by(c)
        query = q_b[span_of(c), window(h, odd)]
        key = [keys_t[columns(h), :seen], lat_t[KVL:, :seen]]
        pad = [jnp.zeros((ROPE, seen), BF16)]
        s_buf[odd, :, :seen] = nn(query, jnp.concatenate(pad + key if odd else key + pad, 0))

    def softmax_stage(c, h, odd):
        seen = seen_by(c)
        dp_buf[odd, :, :seen] = nn(do_ref[span_of(c), columns(h)], values_t[columns(h), :seen])
        for sub, row in pieces(c):
            scores = [s_buf[odd, sub, :rows] + prev_mask]
            if c > 0:
                scores.append(s_buf[odd, sub, rows:seen - part_rows])
            scores.append(s_buf[odd, sub, seen - part_rows:seen] + bias[sub, :])
            scores = jnp.concatenate(scores, 1)
            top = jnp.max(scores, 1, keepdims=True)
            expons = jnp.exp2((scores - top) * F32(SCALE * math.log2(math.e)))
            probs = expons * (F32(1.0) / jnp.sum(expons, 1, keepdims=True))
            p_buf[odd, sub, :seen] = probs
            pb_all[h, row, :seen] = probs.astype(BF16)

    def output_stage(c, h, odd):
        seen = seen_by(c)
        span = span_of(c)
        cols = columns(h)
        result = nt(pb_all[h, span, :seen], values_t[cols, :seen]).astype(BF16)
        out_ref[span, cols] = result
        row_dot = jnp.sum(do_ref[span, cols].astype(F32) * result.astype(F32), 1, keepdims=True)
        for sub, row in pieces(c):
            dscore = p_buf[odd, sub, :seen] * (dp_buf[odd, sub, :seen] - row_dot[sub]) * F32(SCALE)
            ds_all[h, row, :seen] = dscore.astype(BF16)

    def value_gradient(c, h):
        if c + 1 == CHUNKS:
            gv_t[columns(h), :] = nn(dot_t[columns(h), :], pb_all[h]).astype(BF16)

    def key_gradient(c, h, odd):
        if c + 1 == CHUNKS:
            query_t = q_b[:, window(h, odd)].T
            query_t = query_t[ROPE:] if odd else query_t[:WIDTH]
            g_key = nn(query_t, ds_all[h])
            gk_t[columns(h), :] = g_key[:NOPE].astype(BF16)
            krope[...] += g_key[NOPE:].astype(BF16).astype(F32)

    def query_gradient(c, h):
        seen = seen_by(c)
        span = span_of(c)
        key = jnp.concatenate([keys_t[columns(h), :seen], lat_t[KVL:, :seen]], 0)
        q_at = pl.ds(pl.multiple_of(h * WIDTH, ROPE), WIDTH)
        gq_t[q_at, span] = nt(key, ds_all[h, span, :seen]).astype(BF16)

    def attention(c, hooks):
        trips = heads // 2

        def trip(t, stages):
            if "g" in stages:
                for odd in range(2):
                    value_gradient(c, 2 * (t - 3) + odd)
                for odd in range(2):
                    key_gradient(c, 2 * (t - 3) + odd, odd)
                for odd in range(2):
                    query_gradient(c, 2 * (t - 3) + odd)
            if "o" in stages:
                for odd in range(2):
                    output_stage(c, 2 * (t - 2) + odd, odd)
            if "p" in stages:
                for odd in range(2):
                    softmax_stage(c, 2 * (t - 1) + odd, odd)
            if "s" in stages:
                for odd in range(2):
                    score_stage(c, 2 * t + odd, odd)

        trip(0, "s")
        trip(1, "ps")
        trip(2, "ops")

        @pl.loop(3, trips)
        def _(t):
            for i, hook in enumerate(hooks):
                pl.when(t == 3 + ((trips - 3) * (2 * i + 1)) // (2 * len(hooks)))(hook)
            trip(t, "gops")

        trip(trips, "gop")
        trip(trips + 1, "go")
        trip(trips + 2, "g")

    class Reduce:
        def __init__(self, part, out, relay, final, send, relay_recv, final_recv, stage):
            self.part, self.out, self.relay, self.final = part, out, relay, final
            self.send, self.relay_recv, self.final_recv, self.stage = send, relay_recv, final_recv, stage

        def step(self, t):
            adds_left = lax.rem(last - me, 2) == 1
            adds_right = lax.rem(me, 2) == 1
            left_first = jnp.logical_or(jnp.logical_not(adds_left), adds_right)
            first = jnp.where(left_first, me, last - me)
            in_first = t < first
            at = jnp.where(in_first, t, t - first)
            on_left = in_first == left_first
            owner = jnp.where(on_left, at, last - at)
            adds = jnp.where(on_left, adds_left, adds_right)
            outer = jnp.logical_and(jnp.logical_not(adds), jnp.abs(me - owner) > 1)
            stage = self.stage
            stage[...] = self.part(owner)
            out = self.out(owner)

            def send_to(slot, recv, device):
                return copy_of(out, slot, self.send(owner), recv, {"head": device})

            @pl.when(adds)
            def _():
                slot = self.relay(owner)
                copy_of(slot, slot, self.send(owner), self.relay_recv(owner), right).wait_recv()
                stage[...] += slot[...].astype(F32)

            out[...] = stage[...].astype(BF16)

            @pl.when(outer)
            def _():
                send_to(self.relay(owner), self.relay_recv(owner), jnp.where(on_left, me - 1, me + 1)).start()

            @pl.when(jnp.logical_not(outer))
            def _():
                send_to(self.final(me), self.final_recv(me), owner).start()

        def total(self, stage, begin=True, end=True):
            if begin:
                stage[...] = self.part(me)
            if not end:
                return
            for i in range(n_head):
                from_right = (me < i) & ((me == i - 1) if (last - i) % 2 == 0 else (me < i))
                from_left = (me > i) & ((me == i + 1) if i % 2 == 0 else (me > i))

                @pl.when(from_right | from_left)
                def _():
                    slot = self.final(i)
                    copy_of(slot, slot, self.send(i), self.final_recv(i), right).wait_recv()
                    stage[...] += slot[...].astype(F32)

        def finish(self):
            for i in range(n_head):
                @pl.when(me != i)
                def _():
                    slot = self.out(i)
                    copy_of(slot, slot, self.send(i), self.send(i), right).wait_send()

    def query_part(c):
        def part(owner):
            at = pl.multiple_of(owner * q_cols, q_cols)
            return nn(wq[pl.ds(at, q_cols), :], gq_t[:, c * part_rows:(c + 1) * part_rows])

        return part

    def kv_part(c):
        def part(owner):
            return gkv_own[pl.ds(pl.multiple_of(owner * kv_cols, 8), kv_cols), span_of(c)]

        return part

    q_reduces = [
        Reduce(
            query_part(c),
            lambda i, c=c: rq_out.at[c, i],
            lambda i, c=c: rq_right.at[c, i],
            lambda i, c=c: rq_left.at[c, i],
            lambda i, c=c: rq_send.at[c, i],
            lambda i, c=c: rq_rr.at[c, i],
            lambda i, c=c: rq_rl.at[c, i],
            stage_right,
        )
        for c in range(CHUNKS)
    ]
    kv_reduces = [
        Reduce(
            kv_part(c),
            lambda i, c=c: rkv_out.at[c, i],
            lambda i, c=c: rkv_right.at[c, i],
            lambda i, c=c: rkv_left.at[c, i],
            lambda i, c=c: rkv_send.at[c, i],
            lambda i, c=c: rkv_rr.at[c, i],
            lambda i, c=c: rkv_rl.at[c, i],
            gkv_ref.at[:, span_of(c)],
        )
        for c in range(CHUNKS)
    ]

    loads[2].wait()
    turn(wk, wkt)
    if last > 0:
        kv_step(0)
    loads[3].wait()
    turn(wv, wvt)
    clear_unseen()
    krope[...] = jnp.zeros_like(krope)
    loads[4].wait()
    turn(do_ref, dot_t)
    if last > 0:
        q_step(0, 0)
    loads[5].wait()
    own_queries(0)
    for t in range(1, last - 1):
        kv_step(t)
        if t == max(1, last - 2):
            q_gathers[1].start(0)
        add_arrived(0, t - 1)
        q_step(0, t)
    if last > 1:
        add_arrived(0, last - 2)
        kv_step(last - 1)
    assemble([kv_in[i] for i in range(n_head)], rows)
    expand(rows)
    if last > 1:
        q_step(0, last - 1)
    for i in range(n_head):
        copy_of(kv_ref, kv_prev.at[i], p_send.at[i], p_recv.at[i], after).wait_recv()
    assemble([kv_prev[i] for i in range(n_head)], 0)
    expand(0)
    if last > 0:
        q_step(1, 0)
        add_arrived(0, last - 1)
    finish_queries(0)
    attention(0, [functools.partial(q_step, 1, t) for t in range(1, last - 1)])
    if last > 0:
        q_reduces[0].step(0)
    if last > 1:
        q_step(1, last - 1)
    all_queries(1)
    attention(1, [functools.partial(q_reduces[0].step, t) for t in range(1, last)])

    def project(row):
        span = slice(row, row + rows)
        return nn(wk[...], gk_t[:, span]) + nn(wv[...], gv_t[:, span])

    def finish_chunk(c, stage, begin=True):
        q_reduces[c].total(stage, begin)
        gq_ref[span_of(c), :] = stage[...].T

    final = q_reduces[1]
    if last > 0:
        final.step(0)
    back_out[:KVL, :] = project(0).astype(BF16)
    back_out[KVL:, :] = krope[:, :rows].astype(BF16)
    back = copy_of(back_out, back_in, b_send, b_recv, before)
    back.start()
    if last > 1:
        final.step(1)
    gkv_own[:KVL, :] = project(rows)
    gkv_own[KVL:, :] = krope[:, rows:]
    for t in range(2, last):
        final.step(t)
    back.wait_recv()
    gkv_own[...] += back_in[...].astype(F32)
    between = [lambda: finish_chunk(0, stage_own), lambda: final.total(stage_own, end=False)]
    for t in range(last):
        for c in range(CHUNKS):
            kv_reduces[c].step(t)
        if between:
            between.pop(0)()
    for act in between:
        act()
    finish_chunk(1, stage_own, False)
    for c in range(CHUNKS):
        kv_reduces[c].total(gkv_ref.at[:, span_of(c)])

    kv_gather.finish()
    for c in range(CHUNKS):
        kv_reduces[c].finish()
        q_gathers[c].finish()
        q_reduces[c].finish()
    for i in range(n_head):
        copy_of(kv_ref, kv_prev.at[i], p_send.at[i], p_recv.at[i], after).wait_send()
    back.wait_send()


CHUNKS = 2
PIECE = 32


def store(*refs):
    sems = refs[6]
    copies = [pltpu.make_async_copy(refs[i], refs[i + 3], sems.at[i]) for i in range(3)]
    for copy in copies:
        copy.start()
    for copy in copies:
        copy.wait()


def on_device(n_ctx, n_head, q_latent, kv_latent, w_query, w_key, w_value, d_out):
    rows, q_cols = q_latent.shape
    kv_cols = kv_latent.shape[1]
    ql, qw = w_query.shape
    kw = w_key.shape[1]
    kvw = n_head * kv_cols
    heads = kw // NOPE
    part_rows = rows // CHUNKS
    vmem = pl.BlockSpec(memory_space=pltpu.VMEM)
    hbm = pl.BlockSpec(memory_space=pl.ANY)
    dma = pltpu.SemaphoreType.DMA
    some = (n_head,)
    each = (CHUNKS, n_head)
    results = (
        ((rows, kw), BF16),
        ((rows, q_cols), F32),
        ((kv_cols, rows), F32),
    )
    parts = pl.pallas_call(
        functools.partial(kernel, n_ctx, n_head),
        out_shape=tuple(pltpu.VMEM(shape, dtype) for shape, dtype in results),
        in_specs=[hbm] * 6,
        out_specs=(vmem, vmem, vmem),
        scratch_shapes=[
            pltpu.VMEM((rows, q_cols), BF16),
            pltpu.VMEM((kv_cols, rows), BF16),
            pltpu.VMEM((rows, kw), BF16),
            pltpu.VMEM((ql, qw), BF16),
            pltpu.VMEM((KVL, kw), BF16),
            pltpu.VMEM((KVL, kw), BF16),
            pltpu.VMEM((kw, KVL), BF16),
            pltpu.VMEM((kw, KVL), BF16),
            pltpu.VMEM((kw, rows), BF16),
            pltpu.VMEM((CHUNKS, n_head, part_rows, q_cols), BF16),
            pltpu.VMEM((n_head, kv_cols, rows), BF16),
            pltpu.VMEM((n_head, kv_cols, rows), BF16),
            pltpu.VMEM((kvw, 2 * rows), BF16),
            pltpu.VMEM((part_rows, qw), F32),
            pltpu.VMEM((rows, qw), BF16),
            pltpu.VMEM((kw, 2 * rows), BF16),
            pltpu.VMEM((kw, 2 * rows), BF16),
            pltpu.VMEM((2, part_rows, 2 * rows), F32),
            pltpu.VMEM((2, part_rows, 2 * rows), F32),
            pltpu.VMEM((2, part_rows, 2 * rows), F32),
            pltpu.VMEM((heads, rows, 2 * rows), BF16),
            pltpu.VMEM((heads, rows, 2 * rows), BF16),
            pltpu.VMEM((qw, rows), BF16),
            pltpu.VMEM((kw, 2 * rows), BF16),
            pltpu.VMEM((kw, 2 * rows), BF16),
            pltpu.VMEM((ROPE, 2 * rows), F32),
            pltpu.VMEM((kvw, rows), BF16),
            pltpu.VMEM((kvw, rows), BF16),
            pltpu.VMEM((CHUNKS, n_head, q_cols, part_rows), BF16),
            pltpu.VMEM((CHUNKS, n_head, q_cols, part_rows), BF16),
            pltpu.VMEM((CHUNKS, n_head, q_cols, part_rows), BF16),
            pltpu.VMEM((CHUNKS, n_head, kv_cols, part_rows), BF16),
            pltpu.VMEM((CHUNKS, n_head, kv_cols, part_rows), BF16),
            pltpu.VMEM((CHUNKS, n_head, kv_cols, part_rows), BF16),
            pltpu.VMEM((kvw, rows), F32),
            pltpu.VMEM((q_cols, part_rows), F32),
            pltpu.VMEM((q_cols, part_rows), F32),
            pltpu.VMEM((part_rows, part_rows), F32),
            dma((6,)),
            dma(some), dma(some), dma(some),
            dma(each), dma(each), dma(each),
            dma(some), dma(some),
            dma, dma,
            dma(each), dma(each), dma(each),
            dma(each), dma(each), dma(each),
        ],
        compiler_params=pltpu.CompilerParams(
            collective_id=0, has_side_effects=True, vmem_limit_bytes=58 * 1024 * 1024,
        ),
        name="latent_attention",
    )(q_latent, kv_latent.T, d_out, w_query, w_key, w_value)
    out, gq, gkv_t = pl.pallas_call(
        store,
        out_shape=tuple(jax.ShapeDtypeStruct(shape, dtype) for shape, dtype in results),
        in_specs=[vmem] * 3,
        out_specs=(hbm,) * 3,
        scratch_shapes=[dma((3,))],
        name="store_results",
    )(*(pltpu.with_memory_space_constraint(part, pltpu.VMEM) for part in parts))
    return out, gq, gkv_t.T


def solution(mesh):
    return jax.shard_map(
        functools.partial(on_device, mesh.shape["ctx"], mesh.shape["head"]),
        mesh=mesh,
        in_specs=(
            P("ctx", "head"),
            P("ctx", "head"),
            P(None, "head"),
            P(None, "head"),
            P(None, "head"),
            P("ctx", "head"),
        ),
        out_specs=(P("ctx", "head"), P("ctx", "head"), P("ctx", "head")),
        check_vma=False,
    )
```

```python
import functools
import math

import jax
import jax.numpy as jnp
from jax import lax
from jax.experimental import pallas as pl
from jax.experimental.pallas import tpu as pltpu
from jax.sharding import PartitionSpec as P

KVL = 512
ROPE = 64
NOPE = 128
VDIM = 128
WIDTH = NOPE + ROPE
SCALE = WIDTH ** (-0.5)
F32 = jnp.float32
BF16 = jnp.bfloat16
MESH = pl.DeviceIdType.MESH


def nn(a, b):
    return jnp.dot(a, b, preferred_element_type=F32)


def nt(a, b):
    return lax.dot_general(a, b, (((1,), (1,)), ((), ())), preferred_element_type=F32)


def kernel(
    n_ctx, n_head,
    q_hbm, kv_hbm, do_hbm, wq_hbm, wk_hbm, wv_hbm,
    out_ref, gq_ref, gkv_ref,
    q_ref, kv_ref, do_ref, wq, wk, wv, wkt, wvt, dot_t, q_in, kv_in, kv_prev, lat_t, q_acc, q_b,
    keys_t, values_t, s_buf, dp_buf, p_buf, pb_all, ds_all, gq_t, gk_t, gv_t, krope, back_out, back_in,
    rq_out, rq_right, rq_left, rkv_out, rkv_right, rkv_left, gkv_own, stage_right, stage_own,
    bias, w_sem, kv_r, kv_l, kv_recv, q_r, q_l, q_recv, p_send, p_recv,
    b_send, b_recv, rq_send, rq_rr, rq_rl, rkv_send, rkv_rr, rkv_rl,
):
    ctx = lax.axis_index("ctx")
    me = lax.axis_index("head")
    last = n_head - 1
    rows, q_cols = q_ref.shape
    part_rows = rows // CHUNKS
    kv_cols = kv_ref.shape[0]
    heads = wk.shape[1] // NOPE
    after = {"ctx": lax.rem(ctx + 1, n_ctx)}
    before = {"ctx": lax.rem(ctx + n_ctx - 1, n_ctx)}
    right = {"head": jnp.minimum(me + 1, last)}
    left = {"head": jnp.maximum(me - 1, 0)}
    has_right = me < last
    has_left = me > 0

    loads = [
        pltpu.make_async_copy(src, dst, w_sem.at[i])
        for i, (src, dst) in enumerate((
            (kv_hbm, kv_ref), (q_hbm, q_ref), (wk_hbm, wk), (wv_hbm, wv), (do_hbm, do_ref), (wq_hbm, wq),
        ))
    ]
    for load in loads:
        load.start()

    barrier = pltpu.get_barrier_semaphore()

    for peer in range(n_head):
        @pl.when(me != peer)
        def _():
            pl.semaphore_signal(barrier, inc=1, device_id={"head": peer}, device_id_type=MESH)

    pl.semaphore_signal(barrier, inc=1, device_id=after, device_id_type=MESH)
    pl.semaphore_signal(barrier, inc=1, device_id=before, device_id_type=MESH)
    pl.semaphore_wait(barrier, 2 + last)

    def copy_of(src, dst, send_sem, recv_sem, device):
        return pltpu.make_async_remote_copy(
            src_ref=src, dst_ref=dst, send_sem=send_sem, recv_sem=recv_sem,
            device_id=device, device_id_type=MESH,
        )

    class Gather:
        def __init__(self, own, slots, send_r, send_l, recv):
            self.own, self.slots, self.recv = own, slots, recv
            self.send_r, self.send_l = send_r, send_l

        def moves(self, t, act):
            @pl.when(has_right & (me >= t))
            def _():
                owner = me - t
                src = self.own if t == 0 else self.slots(owner)
                act(copy_of(src, self.slots(owner), self.send_r(t), self.recv(owner), right))

            @pl.when(has_left & (me + t <= last))
            def _():
                owner = me + t
                src = self.own if t == 0 else self.slots(owner)
                act(copy_of(src, self.slots(owner), self.send_l(t), self.recv(owner), left))

        def start(self, t):
            if t < last:
                self.moves(t, lambda copy: copy.start())

        def each(self, t, act):
            @pl.when(me - 1 - t >= 0)
            def _():
                act(me - 1 - t)

            @pl.when(me + 1 + t <= last)
            def _():
                act(me + 1 + t)

        def arrive(self, t, act=None):
            def wait(owner):
                slot = self.slots(owner)
                copy_of(slot, slot, self.send_r(0), self.recv(owner), right).wait_recv()
                if act is not None:
                    act(owner)

            self.each(t, wait)
            self.start(t + 1)

        def finish(self):
            for t in range(last):
                self.moves(t, lambda copy: copy.wait_send())

    def pass_on(owner, src):
        copy_of(src, kv_prev.at[owner], p_send.at[owner], p_recv.at[owner], after).start()

    kv_gather = Gather(kv_ref, lambda i: kv_in.at[i], lambda t: kv_r.at[t], lambda t: kv_l.at[t], lambda i: kv_recv.at[i])
    q_gathers = [
        Gather(
            q_ref.at[pl.ds(c * part_rows, part_rows), :],
            lambda i, c=c: q_in.at[c, i],
            lambda t, c=c: q_r.at[c, t],
            lambda t, c=c: q_l.at[c, t],
            lambda i, c=c: q_recv.at[c, i],
        )
        for c in range(CHUNKS)
    ]
    loads[0].wait()
    kv_gather.start(0)
    pass_on(me, kv_ref)
    loads[1].wait()
    q_gathers[0].start(0)
    kv_in[me] = kv_ref[...]
    for c in range(1, CHUNKS):
        q_in[c, me] = q_ref[c * part_rows:(c + 1) * part_rows, :]

    key_pos = lax.broadcasted_iota(jnp.int32, (part_rows, part_rows), 1)
    query_pos = lax.broadcasted_iota(jnp.int32, (part_rows, part_rows), 0)
    bias[...] = jnp.where(key_pos <= query_pos, F32(0.0), F32(-1e30))
    prev_mask = jnp.where(ctx == 0, F32(-1e30), F32(0.0))
    def clear_unseen():
        for c in range(CHUNKS - 1):
            seen = rows + (c + 1) * part_rows
            unseen = jnp.zeros((heads, part_rows, 2 * rows - seen), BF16)
            pb_all[:, c * part_rows:(c + 1) * part_rows, seen:] = unseen
            ds_all[:, c * part_rows:(c + 1) * part_rows, seen:] = unseen

    def turn(src, dst):
        @pl.loop(0, heads // 4)
        def _(j):
            for u in range(4):
                at = pl.multiple_of((4 * j + u) * NOPE, NOPE)
                dst[pl.ds(at, NOPE), :] = src[:, pl.ds(at, NOPE)].T

    def kv_step(t):
        kv_gather.arrive(t, lambda owner: pass_on(owner, kv_in.at[owner]))

    def q_step(c, t):
        q_gathers[c].arrive(t)

    def add_queries(c, block, owner, first=False):
        at = pl.multiple_of(owner * q_cols, q_cols)
        tile = heads * WIDTH

        @pl.loop(0, wq.shape[1] // tile)
        def _(j):
            cols = pl.ds(pl.multiple_of(j * tile, tile), tile)
            part = nn(block[...], wq[pl.ds(at, q_cols), cols])
            if first:
                q_acc[:, cols] = part
            else:
                q_acc[:, cols] += part

    def own_queries(c):
        add_queries(c, q_ref.at[pl.ds(c * part_rows, part_rows), :], me, True)

    def add_arrived(c, t):
        q_gathers[c].each(t, lambda owner: add_queries(c, q_in.at[c, owner], owner))

    def finish_queries(c):
        q_b[c * part_rows:(c + 1) * part_rows, :] = q_acc[...].astype(BF16)

    def all_queries(c):
        tile = 8 * WIDTH

        @pl.loop(0, wq.shape[1] // tile)
        def _(j):
            cols = pl.ds(pl.multiple_of(j * tile, tile), tile)
            if q_cols % 128 == 0:
                total = nn(jnp.concatenate([q_in[c, i] for i in range(n_head)], 1), wq[:, cols])
            else:
                total = nn(q_in[c, 0], wq[:q_cols, cols])
                for i in range(1, n_head):
                    total += nn(q_in[c, i], wq[i * q_cols:(i + 1) * q_cols, cols])
            q_b[c * part_rows:(c + 1) * part_rows, cols] = total.astype(BF16)

    def assemble(parts, row):
        span = slice(row, row + rows)
        if kv_cols % 16 == 0:
            for i in range(n_head):
                lat_t[i * kv_cols:(i + 1) * kv_cols, span] = parts[i]
            return
        width = n_head * kv_cols
        total = None
        for i in range(n_head):
            dst = lax.broadcasted_iota(jnp.int32, (width, kv_cols), 0)
            src = lax.broadcasted_iota(jnp.int32, (width, kv_cols), 1) + i * kv_cols
            place = jnp.where(src == dst, F32(1.0), F32(0.0)).astype(BF16)
            term = nn(place, parts[i])
            total = term if total is None else total + term
        lat_t[:, span] = total.astype(BF16)

    def expand(row):
        tile = 8 * NOPE
        span = slice(row, row + rows)

        @pl.loop(0, heads // 8)
        def _(j):
            cols = pl.ds(pl.multiple_of(j * tile, tile), tile)
            main_t = lat_t[:KVL, span]
            keys_t[cols, span] = nn(wkt[cols, :], main_t).astype(BF16)
            values_t[cols, span] = nn(wvt[cols, :], main_t).astype(BF16)

    def window(h, odd):
        first = (h - 1 if odd else h) * WIDTH + (NOPE if odd else 0)
        return pl.ds(pl.multiple_of(first, NOPE), WIDTH + ROPE)

    def columns(h):
        return pl.ds(pl.multiple_of(h * NOPE, NOPE), NOPE)

    def seen_by(c):
        return rows + (c + 1) * part_rows

    def span_of(c):
        return slice(c * part_rows, (c + 1) * part_rows)

    def pieces(c):
        return [
            (slice(r, r + PIECE), slice(c * part_rows + r, c * part_rows + r + PIECE))
            for r in range(0, part_rows, PIECE)
        ]

    def score_stage(c, h, odd):
        seen = seen_by(c)
        query = q_b[span_of(c), window(h, odd)]
        key = [keys_t[columns(h), :seen], lat_t[KVL:, :seen]]
        pad = [jnp.zeros((ROPE, seen), BF16)]
        s_buf[odd, :, :seen] = nn(query, jnp.concatenate(pad + key if odd else key + pad, 0))

    def softmax_stage(c, h, odd):
        seen = seen_by(c)
        dp_buf[odd, :, :seen] = nn(do_ref[span_of(c), columns(h)], values_t[columns(h), :seen])
        for sub, row in pieces(c):
            scores = [s_buf[odd, sub, :rows] + prev_mask]
            if c > 0:
                scores.append(s_buf[odd, sub, rows:seen - part_rows])
            scores.append(s_buf[odd, sub, seen - part_rows:seen] + bias[sub, :])
            scores = jnp.concatenate(scores, 1)
            top = jnp.max(scores, 1, keepdims=True)
            expons = jnp.exp2((scores - top) * F32(SCALE * math.log2(math.e)))
            probs = expons * (F32(1.0) / jnp.sum(expons, 1, keepdims=True))
            p_buf[odd, sub, :seen] = probs
            pb_all[h, row, :seen] = probs.astype(BF16)

    def output_stage(c, h, odd):
        seen = seen_by(c)
        span = span_of(c)
        cols = columns(h)
        result = nt(pb_all[h, span, :seen], values_t[cols, :seen]).astype(BF16)
        out_ref[span, cols] = result
        row_dot = jnp.sum(do_ref[span, cols].astype(F32) * result.astype(F32), 1, keepdims=True)
        for sub, row in pieces(c):
            dscore = p_buf[odd, sub, :seen] * (dp_buf[odd, sub, :seen] - row_dot[sub]) * F32(SCALE)
            ds_all[h, row, :seen] = dscore.astype(BF16)

    def value_gradient(c, h):
        if c + 1 == CHUNKS:
            gv_t[columns(h), :] = nn(dot_t[columns(h), :], pb_all[h]).astype(BF16)

    def key_gradient(c, h, odd):
        if c + 1 == CHUNKS:
            query_t = q_b[:, window(h, odd)].T
            query_t = query_t[ROPE:] if odd else query_t[:WIDTH]
            g_key = nn(query_t, ds_all[h])
            gk_t[columns(h), :] = g_key[:NOPE].astype(BF16)
            krope[...] += g_key[NOPE:].astype(BF16).astype(F32)

    def query_gradient(c, h):
        seen = seen_by(c)
        span = span_of(c)
        key = jnp.concatenate([keys_t[columns(h), :seen], lat_t[KVL:, :seen]], 0)
        q_at = pl.ds(pl.multiple_of(h * WIDTH, ROPE), WIDTH)
        gq_t[q_at, span] = nt(key, ds_all[h, span, :seen]).astype(BF16)

    def attention(c, hooks):
        trips = heads // 2

        def trip(t, stages):
            if "g" in stages:
                for odd in range(2):
                    value_gradient(c, 2 * (t - 3) + odd)
                for odd in range(2):
                    key_gradient(c, 2 * (t - 3) + odd, odd)
                for odd in range(2):
                    query_gradient(c, 2 * (t - 3) + odd)
            if "o" in stages:
                for odd in range(2):
                    output_stage(c, 2 * (t - 2) + odd, odd)
            if "p" in stages:
                for odd in range(2):
                    softmax_stage(c, 2 * (t - 1) + odd, odd)
            if "s" in stages:
                for odd in range(2):
                    score_stage(c, 2 * t + odd, odd)

        trip(0, "s")
        trip(1, "ps")
        trip(2, "ops")

        @pl.loop(3, trips)
        def _(t):
            for i, hook in enumerate(hooks):
                pl.when(t == 3 + ((trips - 3) * (2 * i + 1)) // (2 * len(hooks)))(hook)
            trip(t, "gops")

        trip(trips, "gop")
        trip(trips + 1, "go")
        trip(trips + 2, "g")

    class Reduce:
        def __init__(self, part, out, relay, final, send, relay_recv, final_recv, stage):
            self.part, self.out, self.relay, self.final = part, out, relay, final
            self.send, self.relay_recv, self.final_recv, self.stage = send, relay_recv, final_recv, stage

        def step(self, t):
            adds_left = lax.rem(last - me, 2) == 1
            adds_right = lax.rem(me, 2) == 1
            left_first = jnp.logical_or(jnp.logical_not(adds_left), adds_right)
            first = jnp.where(left_first, me, last - me)
            in_first = t < first
            at = jnp.where(in_first, t, t - first)
            on_left = in_first == left_first
            owner = jnp.where(on_left, at, last - at)
            adds = jnp.where(on_left, adds_left, adds_right)
            outer = jnp.logical_and(jnp.logical_not(adds), jnp.abs(me - owner) > 1)
            stage = self.stage
            stage[...] = self.part(owner)
            out = self.out(owner)

            def send_to(slot, recv, device):
                return copy_of(out, slot, self.send(owner), recv, {"head": device})

            @pl.when(adds)
            def _():
                slot = self.relay(owner)
                copy_of(slot, slot, self.send(owner), self.relay_recv(owner), right).wait_recv()
                stage[...] += slot[...].astype(F32)

            out[...] = stage[...].astype(BF16)

            @pl.when(outer)
            def _():
                send_to(self.relay(owner), self.relay_recv(owner), jnp.where(on_left, me - 1, me + 1)).start()

            @pl.when(jnp.logical_not(outer))
            def _():
                send_to(self.final(me), self.final_recv(me), owner).start()

        def total(self, stage, begin=True, end=True):
            if begin:
                stage[...] = self.part(me)
            if not end:
                return
            for i in range(n_head):
                from_right = (me < i) & ((me == i - 1) if (last - i) % 2 == 0 else (me < i))
                from_left = (me > i) & ((me == i + 1) if i % 2 == 0 else (me > i))

                @pl.when(from_right | from_left)
                def _():
                    slot = self.final(i)
                    copy_of(slot, slot, self.send(i), self.final_recv(i), right).wait_recv()
                    stage[...] += slot[...].astype(F32)

        def finish(self):
            for i in range(n_head):
                @pl.when(me != i)
                def _():
                    slot = self.out(i)
                    copy_of(slot, slot, self.send(i), self.send(i), right).wait_send()

    def query_part(c):
        def part(owner):
            at = pl.multiple_of(owner * q_cols, q_cols)
            return nn(wq[pl.ds(at, q_cols), :], gq_t[:, c * part_rows:(c + 1) * part_rows])

        return part

    def kv_part(c):
        def part(owner):
            return gkv_own[pl.ds(pl.multiple_of(owner * kv_cols, 8), kv_cols), :]

        return part

    q_reduces = [
        Reduce(
            query_part(c),
            lambda i, c=c: rq_out.at[c, i],
            lambda i, c=c: rq_right.at[c, i],
            lambda i, c=c: rq_left.at[c, i],
            lambda i, c=c: rq_send.at[c, i],
            lambda i, c=c: rq_rr.at[c, i],
            lambda i, c=c: rq_rl.at[c, i],
            stage_right,
        )
        for c in range(CHUNKS)
    ]
    kv_reduces = [
        Reduce(
            kv_part(c),
            lambda i, c=c: rkv_out.at[c, i],
            lambda i, c=c: rkv_right.at[c, i],
            lambda i, c=c: rkv_left.at[c, i],
            lambda i, c=c: rkv_send.at[c, i],
            lambda i, c=c: rkv_rr.at[c, i],
            lambda i, c=c: rkv_rl.at[c, i],
            gkv_ref,
        )
        for c in range(1)
    ]

    loads[2].wait()
    turn(wk, wkt)
    if last > 0:
        kv_step(0)
    loads[3].wait()
    turn(wv, wvt)
    clear_unseen()
    krope[...] = jnp.zeros_like(krope)
    loads[4].wait()
    turn(do_ref, dot_t)
    if last > 0:
        q_step(0, 0)
    loads[5].wait()
    own_queries(0)
    for t in range(1, last - 1):
        kv_step(t)
        if t == max(1, last - 2):
            q_gathers[1].start(0)
        add_arrived(0, t - 1)
        q_step(0, t)
    if last > 1:
        add_arrived(0, last - 2)
        kv_step(last - 1)
    assemble([kv_in[i] for i in range(n_head)], rows)
    expand(rows)
    if last > 1:
        q_step(0, last - 1)
    for i in range(n_head):
        copy_of(kv_ref, kv_prev.at[i], p_send.at[i], p_recv.at[i], after).wait_recv()
    assemble([kv_prev[i] for i in range(n_head)], 0)
    expand(0)
    if last > 0:
        q_step(1, 0)
        add_arrived(0, last - 1)
    finish_queries(0)
    attention(0, [functools.partial(q_step, 1, t) for t in range(1, last - 1)])
    if last > 0:
        q_reduces[0].step(0)
    if last > 1:
        q_step(1, last - 1)
    all_queries(1)
    attention(1, [functools.partial(q_reduces[0].step, t) for t in range(1, last)])

    def project(row):
        span = slice(row, row + rows)
        return nn(wk[...], gk_t[:, span]) + nn(wv[...], gv_t[:, span])

    def finish_chunk(c, stage, begin=True):
        q_reduces[c].total(stage, begin)
        gq_ref[span_of(c), :] = stage[...].T

    final = q_reduces[1]
    if last > 0:
        final.step(0)
    back_out[:KVL, :] = project(0).astype(BF16)
    back_out[KVL:, :] = krope[:, :rows].astype(BF16)
    back = copy_of(back_out, back_in, b_send, b_recv, before)
    back.start()
    if last > 1:
        final.step(1)
    gkv_own[:KVL, :] = project(rows)
    gkv_own[KVL:, :] = krope[:, rows:]
    for t in range(2, last):
        final.step(t)
    back.wait_recv()
    gkv_own[...] += back_in[...].astype(F32)
    between = [lambda: finish_chunk(0, stage_own), lambda: final.total(stage_own, end=False)]
    for t in range(last):
        kv_reduces[0].step(t)
        if between:
            between.pop(0)()
    for act in between:
        act()
    finish_chunk(1, stage_own, False)
    kv_reduces[0].total(gkv_ref)

    kv_gather.finish()
    kv_reduces[0].finish()
    for c in range(CHUNKS):
        q_gathers[c].finish()
        q_reduces[c].finish()
    for i in range(n_head):
        copy_of(kv_ref, kv_prev.at[i], p_send.at[i], p_recv.at[i], after).wait_send()
    back.wait_send()


CHUNKS = 2
PIECE = 32


def store(*refs):
    sems = refs[6]
    copies = [pltpu.make_async_copy(refs[i], refs[i + 3], sems.at[i]) for i in range(3)]
    for copy in copies:
        copy.start()
    for copy in copies:
        copy.wait()


def on_device(n_ctx, n_head, q_latent, kv_latent, w_query, w_key, w_value, d_out):
    rows, q_cols = q_latent.shape
    kv_cols = kv_latent.shape[1]
    ql, qw = w_query.shape
    kw = w_key.shape[1]
    kvw = n_head * kv_cols
    heads = kw // NOPE
    part_rows = rows // CHUNKS
    vmem = pl.BlockSpec(memory_space=pltpu.VMEM)
    hbm = pl.BlockSpec(memory_space=pl.ANY)
    dma = pltpu.SemaphoreType.DMA
    some = (n_head,)
    each = (CHUNKS, n_head)
    results = (
        ((rows, kw), BF16),
        ((rows, q_cols), F32),
        ((kv_cols, rows), F32),
    )
    parts = pl.pallas_call(
        functools.partial(kernel, n_ctx, n_head),
        out_shape=tuple(pltpu.VMEM(shape, dtype) for shape, dtype in results),
        in_specs=[hbm] * 6,
        out_specs=(vmem, vmem, vmem),
        scratch_shapes=[
            pltpu.VMEM((rows, q_cols), BF16),
            pltpu.VMEM((kv_cols, rows), BF16),
            pltpu.VMEM((rows, kw), BF16),
            pltpu.VMEM((ql, qw), BF16),
            pltpu.VMEM((KVL, kw), BF16),
            pltpu.VMEM((KVL, kw), BF16),
            pltpu.VMEM((kw, KVL), BF16),
            pltpu.VMEM((kw, KVL), BF16),
            pltpu.VMEM((kw, rows), BF16),
            pltpu.VMEM((CHUNKS, n_head, part_rows, q_cols), BF16),
            pltpu.VMEM((n_head, kv_cols, rows), BF16),
            pltpu.VMEM((n_head, kv_cols, rows), BF16),
            pltpu.VMEM((kvw, 2 * rows), BF16),
            pltpu.VMEM((part_rows, qw), F32),
            pltpu.VMEM((rows, qw), BF16),
            pltpu.VMEM((kw, 2 * rows), BF16),
            pltpu.VMEM((kw, 2 * rows), BF16),
            pltpu.VMEM((2, part_rows, 2 * rows), F32),
            pltpu.VMEM((2, part_rows, 2 * rows), F32),
            pltpu.VMEM((2, part_rows, 2 * rows), F32),
            pltpu.VMEM((heads, rows, 2 * rows), BF16),
            pltpu.VMEM((heads, rows, 2 * rows), BF16),
            pltpu.VMEM((qw, rows), BF16),
            pltpu.VMEM((kw, 2 * rows), BF16),
            pltpu.VMEM((kw, 2 * rows), BF16),
            pltpu.VMEM((ROPE, 2 * rows), F32),
            pltpu.VMEM((kvw, rows), BF16),
            pltpu.VMEM((kvw, rows), BF16),
            pltpu.VMEM((CHUNKS, n_head, q_cols, part_rows), BF16),
            pltpu.VMEM((CHUNKS, n_head, q_cols, part_rows), BF16),
            pltpu.VMEM((CHUNKS, n_head, q_cols, part_rows), BF16),
            pltpu.VMEM((1, n_head, kv_cols, rows), BF16),
            pltpu.VMEM((1, n_head, kv_cols, rows), BF16),
            pltpu.VMEM((1, n_head, kv_cols, rows), BF16),
            pltpu.VMEM((kvw, rows), F32),
            pltpu.VMEM((q_cols, part_rows), F32),
            pltpu.VMEM((q_cols, part_rows), F32),
            pltpu.VMEM((part_rows, part_rows), F32),
            dma((6,)),
            dma(some), dma(some), dma(some),
            dma(each), dma(each), dma(each),
            dma(some), dma(some),
            dma, dma,
            dma(each), dma(each), dma(each),
            dma(each), dma(each), dma(each),
        ],
        compiler_params=pltpu.CompilerParams(
            collective_id=0, has_side_effects=True, vmem_limit_bytes=58 * 1024 * 1024,
        ),
        name="latent_attention",
    )(q_latent, kv_latent.T, d_out, w_query, w_key, w_value)
    out, gq, gkv_t = pl.pallas_call(
        store,
        out_shape=tuple(jax.ShapeDtypeStruct(shape, dtype) for shape, dtype in results),
        in_specs=[vmem] * 3,
        out_specs=(hbm,) * 3,
        scratch_shapes=[dma((3,))],
        name="store_results",
    )(*(pltpu.with_memory_space_constraint(part, pltpu.VMEM) for part in parts))
    return out, gq, gkv_t.T


def solution(mesh):
    return jax.shard_map(
        functools.partial(on_device, mesh.shape["ctx"], mesh.shape["head"]),
        mesh=mesh,
        in_specs=(
            P("ctx", "head"),
            P("ctx", "head"),
            P(None, "head"),
            P(None, "head"),
            P(None, "head"),
            P("ctx", "head"),
        ),
        out_specs=(P("ctx", "head"), P("ctx", "head"), P("ctx", "head")),
        check_vma=False,
    )
```
